8 devices in a mesh: dp: 1 (over z), tp: 2 (over y), cp: 4 (over x, core).
Axes of the slice: x: 2, y: 2, z: 1, core: 2. Of those that a mesh axis runs over, the one named last changes fastest.
Arguments:
- c_latent: bfloat16 [2048, 512], P(('dp', 'cp'))
- k_rope: bfloat16 [2048, 64], P(('dp', 'cp'))
- q_heads: bfloat16 [2048, 64, 192], P(('dp', 'cp'), 'tp')
- d_out: bfloat16 [2048, 64, 128], P(('dp', 'cp'), 'tp')
- w_uk: bfloat16 [512, 64, 128], P(None, 'tp')
- w_uv: bfloat16 [512, 64, 128], P(None, 'tp')
Outputs:
- output 1: bfloat16 [2048, 64, 128], P(('dp', 'cp'), 'tp')
- output 2: float32 [2048, 64, 192], P(('dp', 'cp'), 'tp')
- output 3: float32 [2048, 512], P(('dp', 'cp'))
- output 4: float32 [2048, 64], P(('dp', 'cp'))
- output 5: float32 [512, 64, 128], P('dp', 'tp')
- output 6: float32 [512, 64, 128], P('dp', 'tp')
All inputs are finite; a program needn't handle non-finite values.
Results may differ from the reference program's by a relative error of at most 0.0147516.
Values are sent between devices in bfloat16 or wider.
A program may use at most 1 GiB of HBM per device.

```python
import jax
import jax.numpy as jnp
from jax import lax

TOK_DEV = 512
CP_SIZE = 4
HEADS = 64
KV_RANK = 512
ROPE_DIM = 64
NOPE_DIM = 128
V_DIM = 128

SEQ_LEN = CP_SIZE * TOK_DEV
HALF_LEN = TOK_DEV // 2
N_PIECES = 2 * CP_SIZE
QK_DIM = NOPE_DIM + ROPE_DIM
NEG_BIG = -1.0e30


def setup_inputs(seed: int = 0, part: int = 0) -> dict:
    base_key = jax.random.key(seed)
    part_key = jax.random.fold_in(base_key, part)
    key_c, key_rope, key_q, key_dout = jax.random.split(part_key, 4)
    key_wk, key_wv = jax.random.split(jax.random.key(seed + 7919), 2)
    c_latent = jax.random.normal(key_c, (SEQ_LEN, KV_RANK), jnp.float32)
    k_rope = jax.random.normal(key_rope, (SEQ_LEN, ROPE_DIM), jnp.float32)
    q_heads = 2.0 * jax.random.normal(key_q, (SEQ_LEN, HEADS, QK_DIM), jnp.float32)
    d_out = jax.random.normal(key_dout, (SEQ_LEN, HEADS, V_DIM), jnp.float32)
    w_uk = jax.random.normal(key_wk, (KV_RANK, HEADS, NOPE_DIM), jnp.float32) * KV_RANK ** -0.5
    w_uv = jax.random.normal(key_wv, (KV_RANK, HEADS, V_DIM), jnp.float32) * KV_RANK ** -0.5
    return {
        'c_latent': c_latent.astype(jnp.bfloat16),
        'k_rope': k_rope.astype(jnp.bfloat16),
        'q_heads': q_heads.astype(jnp.bfloat16),
        'd_out': d_out.astype(jnp.bfloat16),
        'w_uk': w_uk.astype(jnp.bfloat16),
        'w_uv': w_uv.astype(jnp.bfloat16),
    }


def row_positions():
    row_ids = jnp.arange(SEQ_LEN)
    shard_idx = row_ids // TOK_DEV
    within = row_ids % TOK_DEV
    piece_idx = jnp.where(within < HALF_LEN, shard_idx, N_PIECES - 1 - shard_idx)
    return piece_idx * HALF_LEN + within % HALF_LEN


def attend(q_all, knope_all, rope_all, v_all):
    positions = row_positions()
    pos_pieces = positions.reshape(N_PIECES, HALF_LEN)
    qk_scale = QK_DIM ** -0.5

    def head_fn(head_args):
        q_head, knope_head, v_head = head_args
        key_rows = jnp.concatenate([knope_head, rope_all], axis=-1)

        def piece_fn(piece_args):
            q_blk, pos_blk = piece_args
            scores = jnp.dot(q_blk, key_rows.T, preferred_element_type=jnp.float32) * qk_scale
            scores = jnp.where(positions[None, :] <= pos_blk[:, None], scores, NEG_BIG)
            weights = jax.nn.softmax(scores, axis=-1)
            return jnp.dot(weights, v_head, preferred_element_type=jnp.float32)

        out_pieces = lax.map(jax.checkpoint(piece_fn), (q_head.reshape(N_PIECES, HALF_LEN, QK_DIM), pos_pieces))
        return out_pieces.reshape(SEQ_LEN, V_DIM)

    heads_out = lax.map(jax.checkpoint(head_fn), (jnp.transpose(q_all, (1, 0, 2)), jnp.transpose(knope_all, (1, 0, 2)), jnp.transpose(v_all, (1, 0, 2))))
    return jnp.transpose(heads_out, (1, 0, 2))


def reference(c_latent, k_rope, q_heads, d_out, w_uk, w_uv):
    c_wide = c_latent.astype(jnp.float32)
    wk_wide = w_uk.astype(jnp.float32)
    wv_wide = w_uv.astype(jnp.float32)
    knope_all = jnp.einsum('sr,rhd->shd', c_wide, wk_wide).astype(jnp.bfloat16).astype(jnp.float32)
    v_all = jnp.einsum('sr,rhd->shd', c_wide, wv_wide).astype(jnp.bfloat16).astype(jnp.float32)
    out_wide, vjp_fn = jax.vjp(attend, q_heads.astype(jnp.float32), knope_all, k_rope.astype(jnp.float32), v_all)
    dq_heads, dk_nope, dk_rope, dv_all = vjp_fn(d_out.astype(jnp.float32))
    dc_latent = jnp.einsum('shd,rhd->sr', dk_nope, wk_wide) + jnp.einsum('shd,rhd->sr', dv_all, wv_wide)
    dw_uk = jnp.einsum('sr,shd->rhd', c_wide, dk_nope)
    dw_uv = jnp.einsum('sr,shd->rhd', c_wide, dv_all)
    return (out_wide.astype(jnp.bfloat16), dq_heads, dc_latent, dk_rope, dw_uk, dw_uv)
```

```python
import functools
import math

import jax
import jax.numpy as jnp
from jax import lax
from jax.experimental import pallas as pl
from jax.experimental.pallas import tpu as pltpu
from jax.sharding import PartitionSpec as P


NEG_BIG = -1.0e30
PIECE = 256
GROUP = 2
F32 = jnp.float32
BF16 = jnp.bfloat16


def dot(a, b):
    return jnp.dot(a, b, preferred_element_type=F32)


def dot_t(a, b):
    return lax.dot_general(a, b, (((1,), (1,)), ((), ())), preferred_element_type=F32)


def rows(i, n=1):
    return pl.ds(i * PIECE, n * PIECE)


def head_body(lens, scale, c_ref, ct_ref, w_ref, k_s, kt_s, v_s, vt_s, q_s, do_s, s_s, p_s, ds_s,
              o_s, dq_s, dw_ref, dkv_ref, dr_ref):
    n_max = max(lens)
    n_rows = n_max * PIECE
    d_n = v_s.shape[1]
    to_log2 = scale * math.log2(math.e)
    w_t = w_ref[0]
    for j in range(0, n_max, 2):
        kv = dot_t(c_ref[rows(j, 2), :], w_t).astype(BF16)
        k_s[rows(j, 2), 0:d_n] = kv[:, :d_n]
        v_s[rows(j, 2), :] = kv[:, d_n:]
        kv_t = dot(w_t, ct_ref[:, rows(j, 2)]).astype(BF16)
        kt_s[0:d_n, rows(j, 2)] = kv_t[:d_n]
        vt_s[:, rows(j, 2)] = kv_t[d_n:]
    key_i = lax.broadcasted_iota(jnp.int32, (PIECE, PIECE), 0)
    qry_i = lax.broadcasted_iota(jnp.int32, (PIECE, PIECE), 1)
    for b, n in enumerate(lens):
        q_b = q_s[rows(b), :]
        do_b = do_s[rows(b), :]
        top8 = jnp.full((8, PIECE), NEG_BIG, F32)
        for j in range(n):
            s = dot_t(k_s[rows(j), :], q_b)
            if j == n - 1:
                s = jnp.where(key_i <= qry_i, s, NEG_BIG)
            s_s[rows(j), :] = s
            top8 = jnp.maximum(top8, jnp.max(s.reshape(PIECE // 8, 8, PIECE), axis=0))
        top = jnp.max(top8, axis=0, keepdims=True) * to_log2
        sum8 = jnp.zeros((8, PIECE), F32)
        for j in range(n):
            p = jnp.exp2(s_s[rows(j), :] * to_log2 - top)
            sum8 = sum8 + jnp.sum(p.reshape(PIECE // 8, 8, PIECE), axis=0)
            s_s[rows(j), :] = p
            p_s[rows(j), rows(b)] = p.astype(BF16)
        inv = 1.0 / jnp.sum(sum8, axis=0, keepdims=True)
        o_t = dot(vt_s[:, 0:n * PIECE], p_s[0:n * PIECE, rows(b)]) * inv
        o_b = o_t.T
        o_s[rows(b), :] = o_b.astype(BF16)
        d_dot = jnp.sum(o_t * do_b.astype(F32).T, axis=0, keepdims=True)
        for j in range(n):
            dp = dot_t(v_s[rows(j), :], do_b)
            p = s_s[rows(j), :] * inv
            p_s[rows(j), rows(b)] = p.astype(BF16)
            ds_s[rows(j), rows(b)] = (p * (dp - d_dot)).astype(BF16)
        dq_t = dot(kt_s[:, 0:n * PIECE], ds_s[0:n * PIECE, rows(b)]) * scale
        dq_s[rows(b), :] = dq_t.T
    for j in range(n_max):
        w = PIECE * sum(1 for n in lens if n > j)
        dv = dot(p_s[rows(j), 0:w], do_s[0:w, :])
        dk = dot(ds_s[rows(j), 0:w], q_s[0:w, :]) * scale
        dkv_ref[rows(j), 0:d_n] = dk[:, :d_n].astype(BF16)
        dkv_ref[rows(j), d_n:] = dv.astype(BF16)
        dr_ref[rows(j), :] += dk[:, d_n:]
    if n_rows < dkv_ref.shape[0]:
        dkv_ref[n_rows:, :] = jnp.zeros((dkv_ref.shape[0] - n_rows, dkv_ref.shape[1]), BF16)
    dw_ref[0] = dot(ct_ref[:, 0:n_rows], dkv_ref[0:n_rows, :])


def group_kernel(cp_half, scale, n_alias, idx_ref, c_ref, ct_ref, r_ref, rt_ref, w_ref, q_own, q_oth, do_own, do_oth, *rest):
    (o_own, o_oth, dq_own, dq_oth, dkv_ref, dw_ref, dr_ref,
     k_s, kt_s, v_s, vt_s, q_s, do_s, s_s, p_s, ds_s, o_s, dq_s) = rest[n_alias:]
    d_n = v_s.shape[1]
    core = idx_ref[1]

    @pl.when(pl.program_id(0) == 0)
    def _():
        k_s[:, d_n:] = r_ref[...]
        kt_s[d_n:, :] = rt_ref[...]
        dr_ref[...] = jnp.zeros(dr_ref.shape, F32)

    def at(i):
        return pl.ds(pl.multiple_of(i * PIECE, PIECE), PIECE)

    own_hi, own_lo, oth_hi, oth_lo = core, 3 - core, 1 - core, 2 + core
    q_s[at(own_lo), :] = q_own[0, 0:PIECE, :]
    q_s[at(own_hi), :] = q_own[0, PIECE:, :]
    q_s[at(oth_lo), :] = q_oth[0, 0:PIECE, :]
    q_s[at(oth_hi), :] = q_oth[0, PIECE:, :]
    do_s[at(own_lo), :] = do_own[0, 0:PIECE, :]
    do_s[at(own_hi), :] = do_own[0, PIECE:, :]
    do_s[at(oth_lo), :] = do_oth[0, 0:PIECE, :]
    do_s[at(oth_hi), :] = do_oth[0, PIECE:, :]
    n_pieces = 4 * cp_half
    for chip in range(cp_half):
        dev_a, dev_b = 2 * chip, 2 * chip + 1
        lens = (n_pieces - dev_a, n_pieces - dev_b, dev_b + 1, dev_a + 1)
        pl.when(idx_ref[0] == chip)(functools.partial(
            head_body, lens, scale, c_ref, ct_ref, w_ref, k_s, kt_s, v_s, vt_s, q_s, do_s, s_s, p_s, ds_s,
            o_s, dq_s, dw_ref, dkv_ref, dr_ref))
    o_own[0, 0:PIECE, :] = o_s[at(own_lo), :]
    o_own[0, PIECE:, :] = o_s[at(own_hi), :]
    o_oth[0, 0:PIECE, :] = o_s[at(oth_lo), :]
    o_oth[0, PIECE:, :] = o_s[at(oth_hi), :]
    dq_own[0, 0:PIECE, :] = dq_s[at(own_lo), :]
    dq_own[0, PIECE:, :] = dq_s[at(own_hi), :]
    dq_oth[0, 0:PIECE, :] = dq_s[at(oth_lo), :]
    dq_oth[0, PIECE:, :] = dq_s[at(oth_hi), :]


def group_call(first, count, cp_half, scale, idx, c_all, ct_all, r_all, rt_all, w_t, q_all, q_oth, do_all, do_oth, carried):
    seq, rank = c_all.shape
    d_r = r_all.shape[1]
    half_heads, tok, d_qk = q_oth.shape
    d_v = do_oth.shape[2]
    d_n = d_qk - d_r
    kv = w_t.shape[1]
    whole = lambda *shape: pl.BlockSpec(shape, lambda h, idx: (0,) * len(shape))
    mine = lambda *shape: pl.BlockSpec((1,) + shape, lambda h, idx: (idx[1] * half_heads + first + h, 0, 0))
    part = lambda *shape: pl.BlockSpec((1,) + shape, lambda h, idx: (first + h, 0, 0))
    in_specs = [whole(seq, rank), whole(rank, seq), whole(seq, d_r), whole(d_r, seq),
                mine(kv, rank), mine(tok, d_qk), part(tok, d_qk), mine(tok, d_v), part(tok, d_v)]
    out_specs = [part(tok, d_v), part(tok, d_v), part(tok, d_qk), part(tok, d_qk),
                 pl.BlockSpec((seq, kv), lambda h, idx: (0, first + h)),
                 pl.BlockSpec((1, rank, kv), lambda h, idx: (h, 0, 0)),
                 whole(seq, d_r)]
    sds = jax.ShapeDtypeStruct
    out_shape = [sds((half_heads, tok, d_v), BF16), sds((half_heads, tok, d_v), BF16),
                 sds((half_heads, tok, d_qk), F32), sds((half_heads, tok, d_qk), F32),
                 sds((seq, half_heads * kv), BF16), sds((count, rank, kv), F32), sds((seq, d_r), F32)]
    args = [idx, c_all, ct_all, r_all, rt_all, w_t, q_all, q_oth, do_all, do_oth]
    aliases = {}
    for i, arr in enumerate(carried):
        aliases[len(args)] = i
        args.append(arr)
        in_specs.append(pl.BlockSpec(memory_space=pl.ANY))
    pairs = 2 * tok * (seq // 2 + PIECE // 2)
    flops = count * (2 * pairs * (3 * d_qk + 3 * d_v) + 6 * seq * rank * kv)
    return pl.pallas_call(
        functools.partial(group_kernel, cp_half, scale, len(carried)),
        grid_spec=pltpu.PrefetchScalarGridSpec(
            num_scalar_prefetch=1, grid=(count,), in_specs=in_specs, out_specs=out_specs,
            scratch_shapes=[
                pltpu.VMEM((seq, d_qk), BF16), pltpu.VMEM((d_qk, seq), BF16),
                pltpu.VMEM((seq, d_v), BF16), pltpu.VMEM((d_v, seq), BF16),
                pltpu.VMEM((2 * tok, d_qk), BF16), pltpu.VMEM((2 * tok, d_v), BF16),
                pltpu.VMEM((seq, PIECE), F32),
                pltpu.VMEM((seq, 2 * tok), BF16), pltpu.VMEM((seq, 2 * tok), BF16),
                pltpu.VMEM((2 * tok, d_v), BF16), pltpu.VMEM((2 * tok, d_qk), F32)]),
        out_shape=out_shape,
        input_output_aliases=aliases,
        compiler_params=pltpu.CompilerParams(dimension_semantics=("arbitrary",), vmem_limit_bytes=60 * 2 ** 20),
        cost_estimate=pl.CostEstimate(flops=int(flops), bytes_accessed=count * 4 * 2 ** 20, transcendentals=count * pairs),
        name=f"heads_{first}",
    )(*args)


def solution(mesh):
    n_cp = mesh.shape['cp']
    n_tp = mesh.shape['tp']
    cp_half = n_cp // 2
    x_perm = [(d, (d + 2) % n_cp) for d in range(n_cp)]
    core_perm = [(d, d ^ 1) for d in range(n_cp)]
    tp_perm = [(d, (d + 1) % n_tp) for d in range(n_tp)]
    seq_spec = P(('dp', 'cp'), None)
    head_spec = P(('dp', 'cp'), 'tp', None)
    weight_spec = P(None, 'tp', None)
    grad_spec = P('dp', 'tp', None)

    def device_fn(c_latent, k_rope, q_heads, d_out, w_uk, w_uv):
        tok, rank = c_latent.shape
        n_heads = q_heads.shape[1]
        half_heads = n_heads // 2
        d_n = w_uk.shape[2]
        scale = q_heads.shape[2] ** -0.5
        me = lax.axis_index('cp')
        chip, core = me // 2, me % 2
        my_tp = lax.axis_index('tp')
        idx = jnp.stack([chip, core]).astype(jnp.int32)
        swap_x = lambda a: lax.ppermute(a, 'cp', x_perm)
        swap_core = lambda a: lax.ppermute(a, 'cp', core_perm)
        swap_tp = lambda a: lax.ppermute(a, 'tp', tp_perm)

        def gather(own):
            far = swap_x(own)
            near, far_near = swap_core(own), swap_core(far)
            pick = lambda cond, a, b: jnp.where(cond, a, b)
            here = (pick(core == 0, own, near), pick(core == 0, near, own))
            there = (pick(core == 0, far, far_near), pick(core == 0, far_near, far))
            dev = [pick(chip == 0, here[0], there[0]), pick(chip == 0, here[1], there[1]),
                   pick(chip == 0, there[0], here[0]), pick(chip == 0, there[1], here[1])]
            return jnp.concatenate([d[:PIECE] for d in dev] + [d[PIECE:] for d in dev[::-1]], axis=0)

        c_all, r_all = gather(c_latent), gather(k_rope)
        ct_all, rt_all = c_all.T, r_all.T
        w_t = jnp.concatenate([w_uk.transpose(1, 2, 0), w_uv.transpose(1, 2, 0)], axis=1)
        q_all = q_heads.transpose(1, 0, 2)
        do_all = d_out.transpose(1, 0, 2)
        away = (1 - core) * half_heads
        q_oth = swap_core(lax.dynamic_slice_in_dim(q_all, away, half_heads, 0))
        do_oth = swap_core(lax.dynamic_slice_in_dim(do_all, away, half_heads, 0))

        carried, dw_near, dw_far, dr = (), [], [], 0.0
        for first in range(0, half_heads, GROUP):
            outs = group_call(first, GROUP, cp_half, scale, idx, c_all, ct_all, r_all, rt_all, w_t, q_all, q_oth, do_all, do_oth, carried)
            carried = outs[:5]
            dw = outs[5] + swap_x(outs[5])
            dw_near.append(dw)
            dw_far.append(swap_core(dw))
            dr = dr + outs[6]
        o_own, o_oth, dq_own, dq_oth, dkv = carried

        def join(own, oth):
            return jnp.where(core == 0, jnp.concatenate([own, oth], axis=0), jnp.concatenate([oth, own], axis=0)).transpose(1, 0, 2)

        out = join(o_own, swap_core(o_oth))
        dq = join(dq_own, swap_core(dq_oth))
        dw = join(jnp.concatenate(dw_near, axis=0), jnp.concatenate(dw_far, axis=0))

        w_mine = lax.dynamic_slice_in_dim(w_t, core * half_heads, half_heads, 0).reshape(-1, rank)
        dc = dot(dkv, w_mine)
        dcr = jnp.concatenate([dc, dr, jnp.zeros_like(dr)], axis=1)
        lo, hi = dcr[:tok * n_cp // 2].reshape(n_cp, PIECE, -1), dcr[tok * n_cp // 2:].reshape(n_cp, PIECE, -1)[::-1]
        by_dev = jnp.stack([lo, hi], axis=1).reshape(cp_half, 2, 2, PIECE, -1)

        def fold(arr, axis, pos, swap):
            keep = lax.dynamic_index_in_dim(arr, pos, axis, keepdims=False)
            send = lax.dynamic_index_in_dim(arr, 1 - pos, axis, keepdims=False)
            return keep + swap(send)

        part = fold(by_dev, 1, core, swap_core)
        part = fold(part, 1, my_tp, swap_tp)
        part = fold(part, 0, chip, swap_x)
        mate = swap_tp(part)
        full = jnp.where(my_tp == 0, jnp.concatenate([part, mate], axis=0), jnp.concatenate([mate, part], axis=0))
        return (out, dq, full[:, :rank], full[:, rank:rank + k_rope.shape[1]], dw[:, :, :d_n], dw[:, :, d_n:])

    return jax.shard_map(device_fn, mesh=mesh,
                         in_specs=(seq_spec, seq_spec, head_spec, head_spec, weight_spec, weight_spec),
                         out_specs=(head_spec, head_spec, seq_spec, seq_spec, grad_spec, grad_spec),
                         check_vma=False)
```

```python
import functools
import math

import jax
import jax.numpy as jnp
from jax import lax
from jax.experimental import pallas as pl
from jax.experimental.pallas import tpu as pltpu
from jax.sharding import PartitionSpec as P


NEG_BIG = -1.0e30
PIECE = 256
GROUP = 2
BATCH = 8
F32 = jnp.float32
BF16 = jnp.bfloat16


def dot(a, b):
    return jnp.dot(a, b, preferred_element_type=F32)


def dot_t(a, b):
    return lax.dot_general(a, b, (((1,), (1,)), ((), ())), preferred_element_type=F32)


def rows(i, n=1):
    return pl.ds(i * PIECE, n * PIECE)


def params(mib):
    return pltpu.CompilerParams(dimension_semantics=("arbitrary",), vmem_limit_bytes=mib * 2 ** 20)


def head_body(lens, scale, c_ref, ct_ref, w_s, wt_s, k_s, kt_s, v_s, vt_s, qt_s, do_s, s_s, p_s, ds_s,
              o_s, dqt_s, dw_ref, dkv_ref, dr_ref):
    n_max = max(lens)
    n_rows = n_max * PIECE
    d_n = v_s.shape[1]
    to_log2 = scale * math.log2(math.e)
    for j in range(0, n_max, 2):
        kv = dot(c_ref[rows(j, 2), :], w_s[...]).astype(BF16)
        k_s[rows(j, 2), 0:d_n] = kv[:, :d_n]
        v_s[rows(j, 2), :] = kv[:, d_n:]
        kv_t = dot(wt_s[...], ct_ref[:, rows(j, 2)]).astype(BF16)
        kt_s[0:d_n, rows(j, 2)] = kv_t[:d_n]
        vt_s[:, rows(j, 2)] = kv_t[d_n:]
    key_i = lax.broadcasted_iota(jnp.int32, (PIECE, PIECE), 0)
    qry_i = lax.broadcasted_iota(jnp.int32, (PIECE, PIECE), 1)
    for b, n in enumerate(lens):
        qt_b = qt_s[:, rows(b)]
        do_t = do_s[rows(b), :].T
        top8 = jnp.full((8, PIECE), NEG_BIG, F32)
        for j in range(n):
            s = dot(k_s[rows(j), :], qt_b)
            if j == n - 1:
                s = jnp.where(key_i <= qry_i, s, NEG_BIG)
            s_s[rows(j), :] = s
            top8 = jnp.maximum(top8, jnp.max(s.reshape(PIECE // 8, 8, PIECE), axis=0))
        top = jnp.max(top8, axis=0, keepdims=True) * to_log2
        sum8 = jnp.zeros((8, PIECE), F32)
        for j in range(n):
            p = jnp.exp2(s_s[rows(j), :] * to_log2 - top)
            sum8 = sum8 + jnp.sum(p.reshape(PIECE // 8, 8, PIECE), axis=0)
            s_s[rows(j), :] = p
            p_s[rows(j), rows(b)] = p.astype(BF16)
        inv = 1.0 / jnp.sum(sum8, axis=0, keepdims=True)
        o_t = dot(vt_s[:, 0:n * PIECE], p_s[0:n * PIECE, rows(b)]) * inv
        o_s[rows(b), :] = o_t.T.astype(BF16)
        d_dot = jnp.sum(o_t * do_t.astype(F32), axis=0, keepdims=True)
        for j in range(n):
            dp = dot(v_s[rows(j), :], do_t)
            p = s_s[rows(j), :] * inv
            p_s[rows(j), rows(b)] = p.astype(BF16)
            ds_s[rows(j), rows(b)] = (p * (dp - d_dot)).astype(BF16)
        dqt_s[:, rows(b)] = dot(kt_s[:, 0:n * PIECE], ds_s[0:n * PIECE, rows(b)]) * scale
    for j in range(n_max):
        w = PIECE * sum(1 for n in lens if n > j)
        dv = dot(p_s[rows(j), 0:w], do_s[0:w, :])
        dk = dot_t(ds_s[rows(j), 0:w], qt_s[:, 0:w]) * scale
        dkv_ref[rows(j), 0:d_n] = dk[:, :d_n].astype(BF16)
        dkv_ref[rows(j), d_n:] = dv.astype(BF16)
        dr_ref[rows(j), :] += dk[:, d_n:]
    if n_rows < dkv_ref.shape[0]:
        dkv_ref[n_rows:, :] = jnp.zeros((dkv_ref.shape[0] - n_rows, dkv_ref.shape[1]), BF16)
    dw_ref[0] = dot(ct_ref[:, 0:n_rows], dkv_ref[0:n_rows, :])


def group_kernel(cp_half, scale, n_alias, idx_ref, c_ref, ct_ref, r_ref, rt_ref, wk_ref, wv_ref, q_own, q_oth, do_own, do_oth, *rest):
    (o_own, o_oth, dq_own, dq_oth, dkv_ref, dw_ref, dr_ref,
     w_s, wt_s, k_s, kt_s, v_s, vt_s, qt_s, do_s, s_s, p_s, ds_s, o_s, dqt_s) = rest[n_alias:]
    d_n = v_s.shape[1]
    core = idx_ref[1]

    @pl.when(pl.program_id(0) == 0)
    def _():
        k_s[:, d_n:] = r_ref[...]
        kt_s[d_n:, :] = rt_ref[...]
        dr_ref[...] = jnp.zeros(dr_ref.shape, F32)

    w_s[:, 0:d_n] = wk_ref[0]
    w_s[:, d_n:] = wv_ref[0]
    wt_s[0:d_n, :] = wk_ref[0].T
    wt_s[d_n:, :] = wv_ref[0].T

    def at(i):
        return pl.ds(pl.multiple_of(i * PIECE, PIECE), PIECE)

    own_hi, own_lo, oth_hi, oth_lo = core, 3 - core, 1 - core, 2 + core
    lo, hi = pl.ds(0, PIECE), pl.ds(PIECE, PIECE)
    for pos, half, q_ref, do_ref in ((own_lo, lo, q_own, do_own), (own_hi, hi, q_own, do_own),
                                     (oth_lo, lo, q_oth, do_oth), (oth_hi, hi, q_oth, do_oth)):
        qt_s[:, at(pos)] = q_ref[0, :, half]
        do_s[at(pos), :] = do_ref[0, half, :]
    n_pieces = 4 * cp_half
    for chip in range(cp_half):
        dev_a, dev_b = 2 * chip, 2 * chip + 1
        lens = (n_pieces - dev_a, n_pieces - dev_b, dev_b + 1, dev_a + 1)
        pl.when(idx_ref[0] == chip)(functools.partial(
            head_body, lens, scale, c_ref, ct_ref, w_s, wt_s, k_s, kt_s, v_s, vt_s, qt_s, do_s, s_s, p_s, ds_s,
            o_s, dqt_s, dw_ref, dkv_ref, dr_ref))
    for pos, half, o_ref, dq_ref in ((own_lo, lo, o_own, dq_own), (own_hi, hi, o_own, dq_own),
                                     (oth_lo, lo, o_oth, dq_oth), (oth_hi, hi, o_oth, dq_oth)):
        o_ref[0, half, :] = o_s[at(pos), :]
        dq_ref[0, :, half] = dqt_s[:, at(pos)]


sds = jax.ShapeDtypeStruct


def group_call(count, cp_half, scale, idx, c_all, ct_all, r_all, rt_all, w_k, w_v, q_all, q_oth, do_all, do_oth, carried):
    seq, rank = c_all.shape
    d_r = r_all.shape[1]
    half_heads, d_qk, tok = q_oth.shape
    d_v = do_oth.shape[2]
    kv = w_k.shape[2] + w_v.shape[2]
    whole = lambda *shape: pl.BlockSpec(shape, lambda h, idx: (0,) * len(shape))
    mine = lambda *shape: pl.BlockSpec((1,) + shape, lambda h, idx: (idx[1] * half_heads + idx[2] + h, 0, 0))
    part = lambda *shape: pl.BlockSpec((1,) + shape, lambda h, idx: (idx[2] + h, 0, 0))
    in_specs = [whole(seq, rank), whole(rank, seq), whole(seq, d_r), whole(d_r, seq),
                mine(rank, w_k.shape[2]), mine(rank, d_v), mine(d_qk, tok), part(d_qk, tok), mine(tok, d_v), part(tok, d_v)]
    out_specs = [mine(tok, d_v), part(tok, d_v), mine(d_qk, tok), part(d_qk, tok),
                 pl.BlockSpec((seq, kv), lambda h, idx: (0, idx[2] + h)),
                 pl.BlockSpec((1, rank, kv), lambda h, idx: (h, 0, 0)),
                 whole(seq, d_r)]
    out_shape = [sds((2 * half_heads, tok, d_v), BF16), sds((half_heads, tok, d_v), BF16),
                 sds((2 * half_heads, d_qk, tok), F32), sds((half_heads, d_qk, tok), F32),
                 sds((seq, half_heads * kv), BF16), sds((count, rank, kv), F32), sds((seq, d_r), F32)]
    args = [idx, c_all, ct_all, r_all, rt_all, w_k, w_v, q_all, q_oth, do_all, do_oth]
    aliases = {}
    for i, arr in enumerate(carried):
        aliases[len(args)] = i
        args.append(arr)
        in_specs.append(pl.BlockSpec(memory_space=pl.ANY))
    pairs = 2 * tok * (seq // 2 + PIECE // 2)
    flops = count * (2 * pairs * (3 * d_qk + 3 * d_v) + 6 * seq * rank * kv)
    return pl.pallas_call(
        functools.partial(group_kernel, cp_half, scale, len(carried)),
        grid_spec=pltpu.PrefetchScalarGridSpec(
            num_scalar_prefetch=1, grid=(count,), in_specs=in_specs, out_specs=out_specs,
            scratch_shapes=[
                pltpu.VMEM((rank, kv), BF16), pltpu.VMEM((kv, rank), BF16),
                pltpu.VMEM((seq, d_qk), BF16), pltpu.VMEM((d_qk, seq), BF16),
                pltpu.VMEM((seq, d_v), BF16), pltpu.VMEM((d_v, seq), BF16),
                pltpu.VMEM((d_qk, 2 * tok), BF16), pltpu.VMEM((2 * tok, d_v), BF16),
                pltpu.VMEM((seq, PIECE), F32),
                pltpu.VMEM((seq, 2 * tok), BF16), pltpu.VMEM((seq, 2 * tok), BF16),
                pltpu.VMEM((2 * tok, d_v), BF16), pltpu.VMEM((d_qk, 2 * tok), F32)]),
        out_shape=out_shape,
        input_output_aliases=aliases,
        compiler_params=params(48),
        cost_estimate=pl.CostEstimate(flops=int(flops), bytes_accessed=count * 4 * 2 ** 20, transcendentals=count * pairs),
        name="heads",
    )(*args)


def dc_kernel(order, idx_ref, dkv_ref, wk_ref, wv_ref, dr_ref, out_ref, acc_s, w_s):
    rank, d_n = wk_ref.shape[1:]
    w_s[:, 0:d_n] = wk_ref[0]
    w_s[:, d_n:] = wv_ref[0]
    h = pl.program_id(0)

    @pl.when(h == 0)
    def _():
        acc_s[...] = jnp.zeros(acc_s.shape, F32)

    for j in range(len(order)):
        acc_s[rows(j), :] += dot_t(dkv_ref[rows(j), :], w_s[...])

    @pl.when(h == pl.num_programs(0) - 1)
    def _():
        for slot, piece in enumerate(order):
            out_ref[slot, :, 0:rank] = acc_s[rows(piece), :]
            dr = dr_ref[rows(piece), :]
            out_ref[slot, :, rank:] = jnp.concatenate([dr, jnp.zeros_like(dr)], axis=1)


def dc_call(idx, dkv, w_k, w_v, dr, order):
    seq, d_r = dr.shape
    half_heads = w_k.shape[0] // 2
    rank, d_n = w_k.shape[1:]
    kv = d_n + w_v.shape[2]
    mine = lambda *shape: pl.BlockSpec((1,) + shape, lambda h, idx: (idx[1] * half_heads + h, 0, 0))
    shape = (len(order), PIECE, rank + 2 * d_r)
    return pl.pallas_call(
        functools.partial(dc_kernel, order),
        grid_spec=pltpu.PrefetchScalarGridSpec(
            num_scalar_prefetch=1, grid=(half_heads,),
            in_specs=[pl.BlockSpec((seq, kv), lambda h, idx: (0, h)), mine(rank, d_n), mine(rank, d_n),
                      pl.BlockSpec((seq, d_r), lambda h, idx: (0, 0))],
            out_specs=pl.BlockSpec(shape, lambda h, idx: (0, 0, 0)),
            scratch_shapes=[pltpu.VMEM((seq, rank), F32), pltpu.VMEM((rank, kv), BF16)]),
        out_shape=sds(shape, F32),
        compiler_params=params(40),
        cost_estimate=pl.CostEstimate(flops=2 * seq * rank * kv * half_heads, bytes_accessed=30 * 2 ** 20, transcendentals=0),
        name="dc",
    )(idx, dkv, w_k, w_v, dr)


def place_kernel(idx_ref, part_ref, full_ref, out_ref):
    out_ref[...] = part_ref[...]


def place_call(idx, part, full, step):
    n, a, b = part.shape
    return pl.pallas_call(
        place_kernel,
        grid_spec=pltpu.PrefetchScalarGridSpec(
            num_scalar_prefetch=1, grid=(n // step,),
            in_specs=[pl.BlockSpec((step, a, b), lambda h, idx: (h, 0, 0)), pl.BlockSpec(memory_space=pl.ANY)],
            out_specs=pl.BlockSpec((step, a, b), lambda h, idx: ((1 - idx[1]) * (n // step) + h, 0, 0))),
        out_shape=sds(full.shape, full.dtype),
        input_output_aliases={2: 0},
        compiler_params=params(24),
        cost_estimate=pl.CostEstimate(flops=10 ** 9, bytes_accessed=2 * part.size * part.dtype.itemsize, transcendentals=0),
        name="place",
    )(idx, part, full)


def join_kernel(n_parts, idx_ref, *refs):
    a_refs, b_refs = refs[:n_parts], refs[n_parts:2 * n_parts]
    k_ref, v_ref = refs[-2:]
    d_n = k_ref.shape[2]
    for i, (a_ref, b_ref) in enumerate(zip(a_refs, b_refs)):
        for g in range(a_ref.shape[0]):
            s = a_ref[g] + b_ref[g]
            k_ref[:, i * a_ref.shape[0] + g, :] = s[:, :d_n]
            v_ref[:, i * a_ref.shape[0] + g, :] = s[:, d_n:]


def join_call(block, parts_a, parts_b, carried, n_heads):
    g, rank, kv = parts_a[0].shape
    n_parts = len(parts_a)
    r_blk = 128
    part = pl.BlockSpec((g, r_blk, kv), lambda i, idx: (0, i, 0))
    out = pl.BlockSpec((r_blk, g * n_parts, kv // 2), lambda i, idx: (i, idx[0], 0))
    args = [block, *parts_a, *parts_b, *carried]
    return pl.pallas_call(
        functools.partial(join_kernel, n_parts),
        grid_spec=pltpu.PrefetchScalarGridSpec(
            num_scalar_prefetch=1, grid=(rank // r_blk,),
            in_specs=[part] * (2 * n_parts) + [pl.BlockSpec(memory_space=pl.ANY)] * len(carried),
            out_specs=[out, out]),
        out_shape=[sds((rank, n_heads, kv // 2), F32)] * 2,
        input_output_aliases={1 + 2 * n_parts + i: i for i in range(len(carried))},
        compiler_params=params(24),
        cost_estimate=pl.CostEstimate(flops=10 ** 9, bytes_accessed=3 * n_parts * g * rank * kv * 4, transcendentals=0),
        name="join",
    )(*args)


def solution(mesh):
    n_cp = mesh.shape['cp']
    n_tp = mesh.shape['tp']
    cp_half = n_cp // 2
    x_perm = [(d, (d + 2) % n_cp) for d in range(n_cp)]
    core_perm = [(d, d ^ 1) for d in range(n_cp)]
    tp_perm = [(d, (d + 1) % n_tp) for d in range(n_tp)]
    seq_spec = P(('dp', 'cp'), None)
    head_spec = P(('dp', 'cp'), 'tp', None)
    weight_spec = P(None, 'tp', None)
    grad_spec = P('dp', 'tp', None)

    def device_fn(c_latent, k_rope, q_heads, d_out, w_uk, w_uv):
        _, rank = c_latent.shape
        n_heads = q_heads.shape[1]
        half_heads = n_heads // 2
        d_r = k_rope.shape[1]
        scale = q_heads.shape[2] ** -0.5
        me = lax.axis_index('cp')
        chip, core = me // 2, me % 2
        my_tp = lax.axis_index('tp')
        swap_x = lambda a: lax.ppermute(a, 'cp', x_perm)
        swap_core = lambda a: lax.ppermute(a, 'cp', core_perm)
        swap_tp = lambda a: lax.ppermute(a, 'tp', tp_perm)

        def gather(own, axis):
            far = swap_x(own)
            near, far_near = swap_core(own), swap_core(far)
            pick = lambda cond, a, b: jnp.where(cond, a, b)
            here = (pick(core == 0, own, near), pick(core == 0, near, own))
            there = (pick(core == 0, far, far_near), pick(core == 0, far_near, far))
            dev = [pick(chip == 0, here[0], there[0]), pick(chip == 0, here[1], there[1]),
                   pick(chip == 0, there[0], here[0]), pick(chip == 0, there[1], here[1])]
            cut = lambda a, i: lax.slice_in_dim(a, i * PIECE, (i + 1) * PIECE, axis=axis)
            return jnp.concatenate([cut(d, 0) for d in dev] + [cut(d, 1) for d in dev[::-1]], axis=axis)

        c_all, rt_all = gather(c_latent, 0), gather(k_rope.T, 1)
        ct_all, r_all = c_all.T, rt_all.T
        w_k, w_v = w_uk.transpose(1, 0, 2), w_uv.transpose(1, 0, 2)
        q_all = q_heads.transpose(1, 2, 0)
        do_all = d_out.transpose(1, 0, 2)
        away = (1 - core) * half_heads
        q_oth = swap_core(lax.dynamic_slice_in_dim(q_all, away, half_heads, 0))
        do_oth = swap_core(lax.dynamic_slice_in_dim(do_all, away, half_heads, 0))

        n_groups = half_heads // GROUP
        carried, own, far, near, far_near, dr = (), [], [], [], [], 0.0
        for g in range(n_groups):
            idx = jnp.stack([chip, core, jnp.int32(g * GROUP)]).astype(jnp.int32)
            outs = group_call(GROUP, cp_half, scale, idx, c_all, ct_all, r_all, rt_all, w_k, w_v,
                      q_all, q_oth, do_all, do_oth, carried)
            carried = outs[:5]
            own.append(outs[5])
            far.append(swap_x(outs[5]))
            near.append(swap_core(outs[5]))
            far_near.append(swap_core(far[-1]))
            dr = dr + outs[6]
        o_full, o_oth, dq_full, dq_oth, dkv = carried
        idx = jnp.stack([chip, core]).astype(jnp.int32)

        order = [piece for c in range(2) for x in range(cp_half)
                 for piece in (2 * x + c, 2 * n_cp - 1 - 2 * x - c)]
        by_dev = dc_call(idx, dkv, w_k, w_v, dr, order).reshape(2, cp_half, 2, PIECE, -1)
        dq = place_call(idx, swap_core(dq_oth), dq_full, 4).transpose(2, 0, 1)
        out = place_call(idx, swap_core(o_oth), o_full, 8).transpose(1, 0, 2)

        def fold(arr, axis, pos, swap):
            keep = lax.dynamic_index_in_dim(arr, pos, axis, keepdims=False)
            send = lax.dynamic_index_in_dim(arr, 1 - pos, axis, keepdims=False)
            return keep + swap(send)

        part = fold(by_dev, 0, core, swap_core)
        part = fold(part, 1, my_tp, swap_tp)
        part = fold(part, 0, chip, swap_x)
        mate = swap_tp(part)
        full = jnp.where(my_tp == 0, jnp.concatenate([part, mate], axis=0), jnp.concatenate([mate, part], axis=0))

        n_batch = half_heads // BATCH
        per = BATCH // GROUP
        dws = ()
        for i in range(n_batch):
            sel = slice(i * per, (i + 1) * per)
            for side, (a, b) in ((core, (own, far)), (1 - core, (near, far_near))):
                block = (side * n_batch + i).reshape(1).astype(jnp.int32)
                dws = join_call(block, a[sel], b[sel], dws, n_heads)
        return (out, dq, full[:, :rank], full[:, rank:rank + d_r], *dws)

    return jax.shard_map(device_fn, mesh=mesh,
                         in_specs=(seq_spec, seq_spec, head_spec, head_spec, weight_spec, weight_spec),
                         out_specs=(head_spec, head_spec, seq_spec, seq_spec, grad_spec, grad_spec),
                         check_vma=False)
```

```python
import functools
import math

import jax
import jax.numpy as jnp
from jax import lax
from jax.experimental import pallas as pl
from jax.experimental.pallas import tpu as pltpu
from jax.sharding import PartitionSpec as P


NEG_BIG = -1.0e30
PIECE = 256
GROUP = 2
BATCH = 8
F32 = jnp.float32
BF16 = jnp.bfloat16


def dot(a, b):
    return jnp.dot(a, b, preferred_element_type=F32)


def dot_t(a, b):
    return lax.dot_general(a, b, (((1,), (1,)), ((), ())), preferred_element_type=F32)


def rows(i, n=1):
    return pl.ds(i * PIECE, n * PIECE)


def params(mib):
    return pltpu.CompilerParams(dimension_semantics=("arbitrary",), vmem_limit_bytes=mib * 2 ** 20)


def head_body(lens, scale, c_ref, ct_ref, w_s, k_s, kt_s, v_s, vt_s, qt_s, do_s, s_s, p_s, ds_s,
              o_s, dqt_s, dw_ref, dkv_ref, dr_ref):
    n_max = max(lens)
    n_rows = n_max * PIECE
    d_n = v_s.shape[1]
    to_log2 = scale * math.log2(math.e)
    for j in range(0, n_max, 2):
        kv = dot(c_ref[rows(j, 2), :], w_s[...]).astype(BF16)
        k_s[rows(j, 2), 0:d_n] = kv[:, :d_n]
        v_s[rows(j, 2), :] = kv[:, d_n:]
        kt_s[0:d_n, rows(j, 2)] = kv[:, :d_n].T
        vt_s[:, rows(j, 2)] = kv[:, d_n:].T
    key_i = lax.broadcasted_iota(jnp.int32, (PIECE, PIECE), 0)
    qry_i = lax.broadcasted_iota(jnp.int32, (PIECE, PIECE), 1)
    for b, n in enumerate(lens):
        base = sum(lens[:b])
        qt_b = qt_s[:, rows(b)]
        do_t = do_s[rows(b), :].T
        top8 = jnp.full((8, PIECE), NEG_BIG, F32)
        for j in range(n):
            s = dot(k_s[rows(j), :], qt_b)
            if j == n - 1:
                s = jnp.where(key_i <= qry_i, s, NEG_BIG)
            s_s[rows(base + j), :] = s
            top8 = jnp.maximum(top8, jnp.max(s.reshape(PIECE // 8, 8, PIECE), axis=0))
        top = jnp.max(top8, axis=0, keepdims=True) * to_log2
        sum8 = jnp.zeros((8, PIECE), F32)
        for j in range(n):
            p = jnp.exp2(s_s[rows(base + j), :] * to_log2 - top)
            sum8 = sum8 + jnp.sum(p.reshape(PIECE // 8, 8, PIECE), axis=0)
            s_s[rows(base + j), :] = p
            p_s[rows(j), rows(b)] = p.astype(BF16)
        inv = 1.0 / jnp.sum(sum8, axis=0, keepdims=True)
        o_t = dot(vt_s[:, 0:n * PIECE], p_s[0:n * PIECE, rows(b)]) * inv
        o_s[rows(b), :] = o_t.T.astype(BF16)
        d_dot = jnp.sum(o_t * do_t.astype(F32), axis=0, keepdims=True)
        for j in range(n):
            dp = dot(v_s[rows(j), :], do_t)
            p = s_s[rows(base + j), :] * inv
            p_s[rows(j), rows(b)] = p.astype(BF16)
            ds_s[rows(j), rows(b)] = (p * (dp - d_dot)).astype(BF16)
        dqt_s[:, rows(b)] = dot(kt_s[:, 0:n * PIECE], ds_s[0:n * PIECE, rows(b)]) * scale
    for j in range(n_max):
        w = PIECE * sum(1 for n in lens if n > j)
        dv = dot(p_s[rows(j), 0:w], do_s[0:w, :])
        dk = dot_t(ds_s[rows(j), 0:w], qt_s[:, 0:w]) * scale
        dkv_ref[rows(j), 0:d_n] = dk[:, :d_n].astype(BF16)
        dkv_ref[rows(j), d_n:] = dv.astype(BF16)
        dr_ref[rows(j), :] += dk[:, d_n:]
    if n_rows < dkv_ref.shape[0]:
        dkv_ref[n_rows:, :] = jnp.zeros((dkv_ref.shape[0] - n_rows, dkv_ref.shape[1]), BF16)
    dw_ref[0] = dot(ct_ref[:, 0:n_rows], dkv_ref[0:n_rows, :])


def group_kernel(cp_half, scale, n_alias, idx_ref, c_ref, ct_ref, r_ref, rt_ref, wk_ref, wv_ref, q_own, q_oth, do_own, do_oth, *rest):
    (o_own, o_oth, dq_own, dq_oth, dkv_ref, dw_ref, dr_ref,
     w_s, k_s, kt_s, v_s, vt_s, qt_s, do_s, s_s, p_s, ds_s, o_s, dqt_s) = rest[n_alias:]
    d_n = v_s.shape[1]
    core = idx_ref[1]

    @pl.when(pl.program_id(0) == 0)
    def _():
        k_s[:, d_n:] = r_ref[...]
        kt_s[d_n:, :] = rt_ref[...]
        dr_ref[...] = jnp.zeros(dr_ref.shape, F32)

    w_s[:, 0:d_n] = wk_ref[0]
    w_s[:, d_n:] = wv_ref[0]

    def at(i):
        return pl.ds(pl.multiple_of(i * PIECE, PIECE), PIECE)

    own_hi, own_lo, oth_hi, oth_lo = core, 3 - core, 1 - core, 2 + core
    lo, hi = pl.ds(0, PIECE), pl.ds(PIECE, PIECE)
    for pos, half, q_ref, do_ref in ((own_lo, lo, q_own, do_own), (own_hi, hi, q_own, do_own),
                                     (oth_lo, lo, q_oth, do_oth), (oth_hi, hi, q_oth, do_oth)):
        qt_s[:, at(pos)] = q_ref[0, :, half]
        do_s[at(pos), :] = do_ref[0, half, :]
    n_pieces = 4 * cp_half
    for chip in range(cp_half):
        dev_a, dev_b = 2 * chip, 2 * chip + 1
        lens = (n_pieces - dev_a, n_pieces - dev_b, dev_b + 1, dev_a + 1)
        pl.when(idx_ref[0] == chip)(functools.partial(
            head_body, lens, scale, c_ref, ct_ref, w_s, k_s, kt_s, v_s, vt_s, qt_s, do_s, s_s, p_s, ds_s,
            o_s, dqt_s, dw_ref, dkv_ref, dr_ref))
    for pos, half, o_ref, dq_ref in ((own_lo, lo, o_own, dq_own), (own_hi, hi, o_own, dq_own),
                                     (oth_lo, lo, o_oth, dq_oth), (oth_hi, hi, o_oth, dq_oth)):
        o_ref[0, half, :] = o_s[at(pos), :]
        dq_ref[0, :, half] = dqt_s[:, at(pos)]


sds = jax.ShapeDtypeStruct


def group_call(count, cp_half, scale, idx, c_all, ct_all, r_all, rt_all, w_k, w_v, q_all, q_oth, do_all, do_oth, carried):
    seq, rank = c_all.shape
    d_r = r_all.shape[1]
    half_heads, d_qk, tok = q_oth.shape
    d_v = do_oth.shape[2]
    kv = w_k.shape[2] + w_v.shape[2]
    whole = lambda *shape: pl.BlockSpec(shape, lambda h, idx: (0,) * len(shape), pipeline_mode=pl.Buffered(1))
    mine = lambda *shape: pl.BlockSpec((1,) + shape, lambda h, idx: (idx[1] * half_heads + idx[2] + h, 0, 0))
    part = lambda *shape: pl.BlockSpec((1,) + shape, lambda h, idx: (idx[2] + h, 0, 0))
    in_specs = [whole(seq, rank), whole(rank, seq), whole(seq, d_r), whole(d_r, seq),
                mine(rank, w_k.shape[2]), mine(rank, d_v), mine(d_qk, tok), part(d_qk, tok), mine(tok, d_v), part(tok, d_v)]
    out_specs = [mine(tok, d_v), part(tok, d_v), mine(d_qk, tok), part(d_qk, tok),
                 pl.BlockSpec((seq, kv), lambda h, idx: (0, idx[2] + h)),
                 pl.BlockSpec((1, rank, kv), lambda h, idx: (h, 0, 0)),
                 pl.BlockSpec((seq, d_r), lambda h, idx: (0, 0))]
    out_shape = [sds((2 * half_heads, tok, d_v), BF16), sds((half_heads, tok, d_v), BF16),
                 sds((2 * half_heads, d_qk, tok), F32), sds((half_heads, d_qk, tok), F32),
                 sds((seq, half_heads * kv), BF16), sds((count, rank, kv), F32), sds((seq, d_r), F32)]
    args = [idx, c_all, ct_all, r_all, rt_all, w_k, w_v, q_all, q_oth, do_all, do_oth]
    aliases = {}
    for i, arr in enumerate(carried):
        aliases[len(args)] = i
        args.append(arr)
        in_specs.append(pl.BlockSpec(memory_space=pl.ANY))
    pairs = 2 * tok * (seq // 2 + PIECE // 2)
    flops = count * (2 * pairs * (3 * d_qk + 3 * d_v) + 6 * seq * rank * kv)
    return pl.pallas_call(
        functools.partial(group_kernel, cp_half, scale, len(carried)),
        grid_spec=pltpu.PrefetchScalarGridSpec(
            num_scalar_prefetch=1, grid=(count,), in_specs=in_specs, out_specs=out_specs,
            scratch_shapes=[
                pltpu.VMEM((rank, kv), BF16),
                pltpu.VMEM((seq, d_qk), BF16), pltpu.VMEM((d_qk, seq), BF16),
                pltpu.VMEM((seq, d_v), BF16), pltpu.VMEM((d_v, seq), BF16),
                pltpu.VMEM((d_qk, 2 * tok), BF16), pltpu.VMEM((2 * tok, d_v), BF16),
                pltpu.VMEM((seq * 2 + 2 * PIECE, PIECE), F32),
                pltpu.VMEM((seq, 2 * tok), BF16), pltpu.VMEM((seq, 2 * tok), BF16),
                pltpu.VMEM((2 * tok, d_v), BF16), pltpu.VMEM((d_qk, 2 * tok), F32)]),
        out_shape=out_shape,
        input_output_aliases=aliases,
        compiler_params=params(60),
        cost_estimate=pl.CostEstimate(flops=int(flops), bytes_accessed=count * 4 * 2 ** 20, transcendentals=count * pairs),
        name="heads",
    )(*args)


def dc_kernel(order, idx_ref, dkv_ref, wk_ref, wv_ref, *rest):
    out_ref, acc_s, w_s = rest[-3:]
    heads, cols, d_n = wk_ref.shape
    for g in range(heads):
        w_s[:, 2 * g * d_n:(2 * g + 1) * d_n] = wk_ref[g]
        w_s[:, (2 * g + 1) * d_n:(2 * g + 2) * d_n] = wv_ref[g]
    h = pl.program_id(0)

    @pl.when(h == 0)
    def _():
        acc_s[...] = jnp.zeros(acc_s.shape, F32)

    for j in range(0, len(order), 2):
        acc_s[rows(j, 2), :] += dot_t(dkv_ref[rows(j, 2), :], w_s[...])

    @pl.when(h == pl.num_programs(0) - 1)
    def _():
        for slot, piece in enumerate(order):
            out_ref[slot, :, 0:cols] = acc_s[rows(piece), :]
            if len(rest) == 4:
                dr = rest[0][rows(piece), :]
                out_ref[slot, :, cols:] = jnp.concatenate([dr, jnp.zeros_like(dr)], axis=1)


def dc_call(half, idx, dkv, w_k, w_v, extra, order):
    seq = dkv.shape[0]
    half_heads = w_k.shape[0] // 2
    rank, d_n = w_k.shape[1:]
    kv = d_n + w_v.shape[2]
    step = 2
    n_steps = half_heads // step
    w_spec = pl.BlockSpec((step, rank // 2, d_n), lambda h, idx: (idx[1] * n_steps + h, half, 0))
    shape = (len(order), PIECE, rank // 2 + sum(2 * e.shape[1] for e in extra))
    return pl.pallas_call(
        functools.partial(dc_kernel, order),
        grid_spec=pltpu.PrefetchScalarGridSpec(
            num_scalar_prefetch=1, grid=(n_steps,),
            in_specs=[pl.BlockSpec((seq, step * kv), lambda h, idx: (0, h)), w_spec, w_spec]
            + [pl.BlockSpec(e.shape, lambda h, idx: (0, 0)) for e in extra],
            out_specs=pl.BlockSpec(shape, lambda h, idx: (0, 0, 0)),
            scratch_shapes=[pltpu.VMEM((seq, rank // 2), F32), pltpu.VMEM((rank // 2, step * kv), BF16)]),
        out_shape=sds(shape, F32),
        compiler_params=params(60),
        cost_estimate=pl.CostEstimate(flops=seq * rank * kv * half_heads, bytes_accessed=25 * 2 ** 20, transcendentals=0),
        name="dc",
    )(idx, dkv, w_k, w_v, *extra)


def place_kernel(idx_ref, part_ref, full_ref, out_ref):
    out_ref[...] = part_ref[...]


def place_call(idx, part, full, step):
    n, a, b = part.shape
    return pl.pallas_call(
        place_kernel,
        grid_spec=pltpu.PrefetchScalarGridSpec(
            num_scalar_prefetch=1, grid=(n // step,),
            in_specs=[pl.BlockSpec((step, a, b), lambda h, idx: (h, 0, 0)), pl.BlockSpec(memory_space=pl.ANY)],
            out_specs=pl.BlockSpec((step, a, b), lambda h, idx: ((1 - idx[1]) * (n // step) + h, 0, 0))),
        out_shape=sds(full.shape, full.dtype),
        input_output_aliases={2: 0},
        compiler_params=params(24),
        cost_estimate=pl.CostEstimate(flops=10 ** 9, bytes_accessed=2 * part.size * part.dtype.itemsize, transcendentals=0),
        name="place",
    )(idx, part, full)


def join_kernel(n_parts, idx_ref, *refs):
    a_refs, b_refs = refs[:n_parts], refs[n_parts:2 * n_parts]
    k_ref, v_ref = refs[-2:]
    d_n = k_ref.shape[2]
    for i, (a_ref, b_ref) in enumerate(zip(a_refs, b_refs)):
        for g in range(a_ref.shape[0]):
            s = a_ref[g] + b_ref[g]
            k_ref[:, i * a_ref.shape[0] + g, :] = s[:, :d_n]
            v_ref[:, i * a_ref.shape[0] + g, :] = s[:, d_n:]


def join_call(block, parts_a, parts_b, carried, n_heads):
    g, rank, kv = parts_a[0].shape
    n_parts = len(parts_a)
    r_blk = 128
    part = pl.BlockSpec((g, r_blk, kv), lambda i, idx: (0, i, 0))
    out = pl.BlockSpec((r_blk, g * n_parts, kv // 2), lambda i, idx: (i, idx[0], 0))
    args = [block, *parts_a, *parts_b, *carried]
    return pl.pallas_call(
        functools.partial(join_kernel, n_parts),
        grid_spec=pltpu.PrefetchScalarGridSpec(
            num_scalar_prefetch=1, grid=(rank // r_blk,),
            in_specs=[part] * (2 * n_parts) + [pl.BlockSpec(memory_space=pl.ANY)] * len(carried),
            out_specs=[out, out]),
        out_shape=[sds((rank, n_heads, kv // 2), F32)] * 2,
        input_output_aliases={1 + 2 * n_parts + i: i for i in range(len(carried))},
        compiler_params=params(24),
        cost_estimate=pl.CostEstimate(flops=10 ** 9, bytes_accessed=3 * n_parts * g * rank * kv * 4, transcendentals=0),
        name="join",
    )(*args)


def solution(mesh):
    n_cp = mesh.shape['cp']
    n_tp = mesh.shape['tp']
    cp_half = n_cp // 2
    x_perm = [(d, (d + 2) % n_cp) for d in range(n_cp)]
    core_perm = [(d, d ^ 1) for d in range(n_cp)]
    tp_perm = [(d, (d + 1) % n_tp) for d in range(n_tp)]
    seq_spec = P(('dp', 'cp'), None)
    head_spec = P(('dp', 'cp'), 'tp', None)
    weight_spec = P(None, 'tp', None)
    grad_spec = P('dp', 'tp', None)

    def device_fn(c_latent, k_rope, q_heads, d_out, w_uk, w_uv):
        _, rank = c_latent.shape
        n_heads = q_heads.shape[1]
        half_heads = n_heads // 2
        d_r = k_rope.shape[1]
        scale = q_heads.shape[2] ** -0.5
        me = lax.axis_index('cp')
        chip, core = me // 2, me % 2
        my_tp = lax.axis_index('tp')
        swap_x = lambda a: lax.ppermute(a, 'cp', x_perm)
        swap_core = lambda a: lax.ppermute(a, 'cp', core_perm)
        swap_tp = lambda a: lax.ppermute(a, 'tp', tp_perm)

        def gather(own, axis):
            far = swap_x(own)
            near, far_near = swap_core(own), swap_core(far)
            pick = lambda cond, a, b: jnp.where(cond, a, b)
            here = (pick(core == 0, own, near), pick(core == 0, near, own))
            there = (pick(core == 0, far, far_near), pick(core == 0, far_near, far))
            dev = [pick(chip == 0, here[0], there[0]), pick(chip == 0, here[1], there[1]),
                   pick(chip == 0, there[0], here[0]), pick(chip == 0, there[1], here[1])]
            cut = lambda a, i: lax.slice_in_dim(a, i * PIECE, (i + 1) * PIECE, axis=axis)
            return jnp.concatenate([cut(d, 0) for d in dev] + [cut(d, 1) for d in dev[::-1]], axis=axis)

        c_all, rt_all = gather(c_latent, 0), gather(k_rope.T, 1)
        ct_all, r_all = c_all.T, rt_all.T
        w_k, w_v = w_uk.transpose(1, 0, 2), w_uv.transpose(1, 0, 2)
        q_all = q_heads.transpose(1, 2, 0)
        do_all = d_out.transpose(1, 0, 2)
        away = (1 - core) * half_heads
        q_oth = swap_core(lax.dynamic_slice_in_dim(q_all, away, half_heads, 0))
        do_oth = swap_core(lax.dynamic_slice_in_dim(do_all, away, half_heads, 0))

        n_groups = half_heads // GROUP
        carried, own, far, near, far_near, dr = (), [], [], [], [], 0.0
        for g in range(n_groups):
            idx = jnp.stack([chip, core, jnp.int32(g * GROUP)]).astype(jnp.int32)
            outs = group_call(GROUP, cp_half, scale, idx, c_all, ct_all, r_all, rt_all, w_k, w_v,
                      q_all, q_oth, do_all, do_oth, carried)
            carried = outs[:5]
            own.append(outs[5])
            far.append(swap_x(outs[5]))
            near.append(swap_core(outs[5]))
            far_near.append(swap_core(far[-1]))
            dr = dr + outs[6]
        o_full, o_oth, dq_full, dq_oth, dkv = carried
        idx = jnp.stack([chip, core]).astype(jnp.int32)

        order = [piece for c in range(2) for x in range(cp_half)
                 for piece in (2 * x + c, 2 * n_cp - 1 - 2 * x - c)]

        def fold(arr, axis, pos, swap):
            keep = lax.dynamic_index_in_dim(arr, pos, axis, keepdims=False)
            send = lax.dynamic_index_in_dim(arr, 1 - pos, axis, keepdims=False)
            return keep + swap(send)

        full = []
        for half, extra in ((0, ()), (1, (dr,))):
            part = dc_call(half, idx, dkv, w_k, w_v, extra, order).reshape(2, cp_half, 2, PIECE, -1)
            part = fold(part, 0, core, swap_core)
            part = fold(part, 1, my_tp, swap_tp)
            part = fold(part, 0, chip, swap_x)
            mate = swap_tp(part)
            full.append(jnp.where(my_tp == 0, jnp.concatenate([part, mate], axis=0), jnp.concatenate([mate, part], axis=0)))
        dc = jnp.concatenate([full[0], full[1][:, :rank // 2]], axis=1)
        dr_out = full[1][:, rank // 2:rank // 2 + d_r]

        n_batch = half_heads // BATCH
        per = BATCH // GROUP
        dws = ()
        for i in range(n_batch):
            sel = slice(i * per, (i + 1) * per)
            for side, a, b in ((core, own, far), (1 - core, near, far_near)):
                block = (side * n_batch + i).reshape(1).astype(jnp.int32)
                dws = join_call(block, a[sel], b[sel], dws, n_heads)
        dq = place_call(idx, swap_core(dq_oth), dq_full, 4).transpose(2, 0, 1)
        out = place_call(idx, swap_core(o_oth), o_full, 8).transpose(1, 0, 2)
        return (out, dq, dc, dr_out, *dws)

    return jax.shard_map(device_fn, mesh=mesh,
                         in_specs=(seq_spec, seq_spec, head_spec, head_spec, weight_spec, weight_spec),
                         out_specs=(head_spec, head_spec, seq_spec, seq_spec, grad_spec, grad_spec),
                         check_vma=False)
```

```python
import functools
import math

import jax
import jax.numpy as jnp
from jax import lax
from jax.experimental import pallas as pl
from jax.experimental.pallas import tpu as pltpu
from jax.sharding import PartitionSpec as P


NEG_BIG = -1.0e30
PIECE = 256
GROUPS = ((2, 3, 3), (4, 4))
F32 = jnp.float32
BF16 = jnp.bfloat16


def dot(a, b):
    return jnp.dot(a, b, preferred_element_type=F32)


def dot_t(a, b):
    return lax.dot_general(a, b, (((1,), (1,)), ((), ())), preferred_element_type=F32)


def rows(i, n=1):
    return pl.ds(i * PIECE, n * PIECE)


def params(mib):
    return pltpu.CompilerParams(dimension_semantics=("arbitrary",), vmem_limit_bytes=mib * 2 ** 20)


def head_body(lens, scale, c_ref, ct_ref, w_s, k_s, kt_s, v_s, vt_s, qt_s, do_s, s_s, p_s, ds_s,
              o_s, dqt_s, dw_ref, dkv_ref, dr_ref):
    n_max = max(lens)
    n_rows = n_max * PIECE
    d_n = v_s.shape[1]
    to_log2 = scale * math.log2(math.e)
    for j in range(0, n_max, 2):
        kv = dot(c_ref[rows(j, 2), :], w_s[...]).astype(BF16)
        k_s[rows(j, 2), 0:d_n] = kv[:, :d_n]
        v_s[rows(j, 2), :] = kv[:, d_n:]
        kt_s[0:d_n, rows(j, 2)] = kv[:, :d_n].T
        vt_s[:, rows(j, 2)] = kv[:, d_n:].T
    key_i = lax.broadcasted_iota(jnp.int32, (PIECE, PIECE), 0)
    qry_i = lax.broadcasted_iota(jnp.int32, (PIECE, PIECE), 1)
    for b, n in enumerate(lens):
        base = sum(lens[:b])
        qt_b = qt_s[:, rows(b)]
        do_t = do_s[rows(b), :].T
        top8 = jnp.full((8, PIECE), NEG_BIG, F32)
        for j in range(n):
            s = dot(k_s[rows(j), :], qt_b)
            if j == n - 1:
                s = jnp.where(key_i <= qry_i, s, NEG_BIG)
            s_s[rows(base + j), :] = s
            top8 = jnp.maximum(top8, jnp.max(s.reshape(PIECE // 8, 8, PIECE), axis=0))
        top = jnp.max(top8, axis=0, keepdims=True) * to_log2
        sum8 = jnp.zeros((8, PIECE), F32)
        for j in range(n):
            p = jnp.exp2(s_s[rows(base + j), :] * to_log2 - top)
            sum8 = sum8 + jnp.sum(p.reshape(PIECE // 8, 8, PIECE), axis=0)
            s_s[rows(base + j), :] = p
            p_s[rows(j), rows(b)] = p.astype(BF16)
        inv = 1.0 / jnp.sum(sum8, axis=0, keepdims=True)
        o_t = dot(vt_s[:, 0:n * PIECE], p_s[0:n * PIECE, rows(b)]) * inv
        o_s[rows(b), :] = o_t.T.astype(BF16)
        d_dot = jnp.sum(o_t * do_t.astype(F32), axis=0, keepdims=True)
        for j in range(n):
            dp = dot(v_s[rows(j), :], do_t)
            p = s_s[rows(base + j), :] * inv
            p_s[rows(j), rows(b)] = p.astype(BF16)
            ds_s[rows(j), rows(b)] = (p * (dp - d_dot)).astype(BF16)
        dqt_s[:, rows(b)] = dot(kt_s[:, 0:n * PIECE], ds_s[0:n * PIECE, rows(b)]) * scale
    for j in range(n_max):
        w = PIECE * sum(1 for n in lens if n > j)
        dv = dot(p_s[rows(j), 0:w], do_s[0:w, :])
        dk = dot_t(ds_s[rows(j), 0:w], qt_s[:, 0:w]) * scale
        dkv_ref[rows(j), 0:d_n] = dk[:, :d_n].astype(BF16)
        dkv_ref[rows(j), d_n:] = dv.astype(BF16)
        dr_ref[rows(j), :] += dk[:, d_n:]
    if n_rows < dkv_ref.shape[0]:
        dkv_ref[n_rows:, :] = jnp.zeros((dkv_ref.shape[0] - n_rows, dkv_ref.shape[1]), BF16)
    dw_ref[0] = dot(ct_ref[:, 0:n_rows], dkv_ref[0:n_rows, :])


def group_kernel(cp_half, scale, n_alias, idx_ref, c_ref, ct_ref, r_ref, rt_ref, wk_ref, wv_ref, q_own, q_oth, do_own, do_oth, *rest):
    (o_own, o_oth, dq_own, dq_oth, dkv_ref, dr_ref, dw_ref,
     w_s, k_s, kt_s, v_s, vt_s, qt_s, do_s, s_s, p_s, ds_s, o_s, dqt_s) = rest[n_alias:]
    d_n = v_s.shape[1]
    core = idx_ref[1]

    @pl.when(pl.program_id(0) == 0)
    def _():
        k_s[:, d_n:] = r_ref[...]
        kt_s[d_n:, :] = rt_ref[...]
        dr_ref[...] = rest[n_alias - 1][...] if n_alias else jnp.zeros(dr_ref.shape, F32)

    w_s[:, 0:d_n] = wk_ref[0]
    w_s[:, d_n:] = wv_ref[0]

    def at(i):
        return pl.ds(pl.multiple_of(i * PIECE, PIECE), PIECE)

    own_hi, own_lo, oth_hi, oth_lo = core, 3 - core, 1 - core, 2 + core
    lo, hi = pl.ds(0, PIECE), pl.ds(PIECE, PIECE)
    for pos, half, q_ref, do_ref in ((own_lo, lo, q_own, do_own), (own_hi, hi, q_own, do_own),
                                     (oth_lo, lo, q_oth, do_oth), (oth_hi, hi, q_oth, do_oth)):
        qt_s[:, at(pos)] = q_ref[0, :, half]
        do_s[at(pos), :] = do_ref[0, half, :]
    n_pieces = 4 * cp_half
    for chip in range(cp_half):
        dev_a, dev_b = 2 * chip, 2 * chip + 1
        lens = (n_pieces - dev_a, n_pieces - dev_b, dev_b + 1, dev_a + 1)
        pl.when(idx_ref[0] == chip)(functools.partial(
            head_body, lens, scale, c_ref, ct_ref, w_s, k_s, kt_s, v_s, vt_s, qt_s, do_s, s_s, p_s, ds_s,
            o_s, dqt_s, dw_ref, dkv_ref, dr_ref))
    for pos, half, o_ref, dq_ref in ((own_lo, lo, o_own, dq_own), (own_hi, hi, o_own, dq_own),
                                     (oth_lo, lo, o_oth, dq_oth), (oth_hi, hi, o_oth, dq_oth)):
        o_ref[0, half, :] = o_s[at(pos), :]
        dq_ref[0, :, half] = dqt_s[:, at(pos)]


sds = jax.ShapeDtypeStruct


def group_call(count, cp_half, scale, idx, c_all, ct_all, r_all, rt_all, w_k, w_v, q_all, q_oth, do_all, do_oth, carried):
    seq, rank = c_all.shape
    d_r = r_all.shape[1]
    half_heads, d_qk, tok = q_oth.shape
    d_v = do_oth.shape[2]
    kv = w_k.shape[2] + w_v.shape[2]
    whole = lambda *shape: pl.BlockSpec(shape, lambda h, idx: (0,) * len(shape), pipeline_mode=pl.Buffered(1))
    mine = lambda *shape: pl.BlockSpec((1,) + shape, lambda h, idx: (idx[1] * half_heads + idx[2] + h, 0, 0))
    part = lambda *shape: pl.BlockSpec((1,) + shape, lambda h, idx: (idx[2] + h, 0, 0))
    in_specs = [whole(seq, rank), whole(rank, seq), whole(seq, d_r), whole(d_r, seq),
                part(rank, w_k.shape[2]), part(rank, d_v), mine(d_qk, tok), part(d_qk, tok), part(tok, d_v), part(tok, d_v)]
    out_specs = [part(tok, d_v), part(tok, d_v), mine(d_qk, tok), part(d_qk, tok),
                 pl.BlockSpec((seq, kv), lambda h, idx: (0, idx[2] + h)),
                 pl.BlockSpec((seq, d_r), lambda h, idx: (0, 0)),
                 pl.BlockSpec((1, rank, kv), lambda h, idx: (h, 0, 0))]
    out_shape = [sds((half_heads, tok, d_v), BF16), sds((half_heads, tok, d_v), BF16),
                 sds((2 * half_heads, d_qk, tok), F32), sds((half_heads, d_qk, tok), F32),
                 sds((seq, half_heads * kv), BF16), sds((seq, d_r), F32), sds((count, rank, kv), F32)]
    args = [idx, c_all, ct_all, r_all, rt_all, w_k, w_v, q_all, q_oth, do_all, do_oth]
    aliases = {}
    for i, arr in enumerate(carried):
        aliases[len(args)] = i
        args.append(arr)
        in_specs.append(pl.BlockSpec(memory_space=pl.ANY))
    if carried:
        in_specs[-1] = whole(seq, d_r)
    pairs = 2 * tok * (seq // 2 + PIECE // 2)
    flops = count * (2 * pairs * (3 * d_qk + 3 * d_v) + 6 * seq * rank * kv)
    return pl.pallas_call(
        functools.partial(group_kernel, cp_half, scale, len(carried)),
        grid_spec=pltpu.PrefetchScalarGridSpec(
            num_scalar_prefetch=1, grid=(count,), in_specs=in_specs, out_specs=out_specs,
            scratch_shapes=[
                pltpu.VMEM((rank, kv), BF16),
                pltpu.VMEM((seq, d_qk), BF16), pltpu.VMEM((d_qk, seq), BF16),
                pltpu.VMEM((seq, d_v), BF16), pltpu.VMEM((d_v, seq), BF16),
                pltpu.VMEM((d_qk, 2 * tok), BF16), pltpu.VMEM((2 * tok, d_v), BF16),
                pltpu.VMEM((seq * 2 + 2 * PIECE, PIECE), F32),
                pltpu.VMEM((seq, 2 * tok), BF16), pltpu.VMEM((seq, 2 * tok), BF16),
                pltpu.VMEM((2 * tok, d_v), BF16), pltpu.VMEM((d_qk, 2 * tok), F32)]),
        out_shape=out_shape,
        input_output_aliases=aliases,
        compiler_params=params(60),
        cost_estimate=pl.CostEstimate(flops=int(flops), bytes_accessed=count * 4 * 2 ** 20, transcendentals=count * pairs),
        name="heads",
    )(*args)


def dc_kernel(idx_ref, lo_ref, hi_ref, wk_ref, wv_ref, dr_lo, dr_hi, a_ref, b_ref, w_s):
    heads, _, d_n = wk_ref.shape
    cols = a_ref.shape[3]

    @pl.when(pl.program_id(0) == 0)
    def _():
        for g in range(heads):
            w_s[:, 2 * g * d_n:(2 * g + 1) * d_n] = wk_ref[g]
            w_s[:, (2 * g + 1) * d_n:(2 * g + 2) * d_n] = wv_ref[g]

    for j in range(2):
        for k, dkv_ref in enumerate((lo_ref, hi_ref)):
            (a_ref, b_ref)[j][0, k, :, 0:cols] = dot_t(dkv_ref[...], w_s[rows(j), :])
    for k, dr_ref in enumerate((dr_lo, dr_hi)):
        dr = dr_ref[...]
        b_ref[0, k, :, cols:] = jnp.concatenate([dr, jnp.zeros_like(dr)], axis=1)


def dc_call(idx, dkv, w_k, w_v, dr):
    seq, d_r = dr.shape
    half_heads, rank, d_n = w_k.shape
    kv = d_n + w_v.shape[2]
    n = seq // (2 * PIECE)
    dev = lambda i: 2 * (i % (n // 2)) + i // (n // 2)
    lo = lambda w: pl.BlockSpec((PIECE, w), lambda i, idx: (dev(i), 0))
    hi = lambda w: pl.BlockSpec((PIECE, w), lambda i, idx: (2 * n - 1 - dev(i), 0))
    w_spec = pl.BlockSpec((half_heads, rank, d_n), lambda i, idx: (0, 0, 0), pipeline_mode=pl.Buffered(1))
    shapes = [(n, 2, PIECE, rank // 2), (n, 2, PIECE, rank // 2 + 2 * d_r)]
    return pl.pallas_call(
        dc_kernel,
        grid_spec=pltpu.PrefetchScalarGridSpec(
            num_scalar_prefetch=1, grid=(n,),
            in_specs=[lo(half_heads * kv), hi(half_heads * kv), w_spec, w_spec, lo(d_r), hi(d_r)],
            out_specs=[pl.BlockSpec((1,) + s[1:], lambda i, idx: (i, 0, 0, 0)) for s in shapes],
            scratch_shapes=[pltpu.VMEM((rank, half_heads * kv), BF16)]),
        out_shape=[sds(s, F32) for s in shapes],
        compiler_params=params(60),
        cost_estimate=pl.CostEstimate(flops=2 * seq * rank * kv * half_heads, bytes_accessed=30 * 2 ** 20, transcendentals=0),
        name="dc",
    )(idx, dkv, dkv, w_k, w_v, dr, dr)


def gather_kernel(n_dev, idx_ref, *refs):
    c_refs, r_refs = refs[0:4], refs[4:8]
    c_all, ct_all, r_all, rt_all = refs[8:]
    chip, core = idx_ref[0], idx_ref[1]
    devs = (2 * chip + core, 2 * chip + 1 - core, 2 - 2 * chip + core, 3 - 2 * chip - core)
    for dev, c_ref, r_ref in zip(devs, c_refs, r_refs):
        for piece, half in ((dev, rows(0)), (2 * n_dev - 1 - dev, rows(1))):
            at = pl.ds(pl.multiple_of(piece * PIECE, PIECE), PIECE)
            c = c_ref[half, :]
            c_all[at, :] = c
            ct_all[:, at] = c.T
            r = r_ref[:, half]
            rt_all[:, at] = r
            r_all[at, :] = r.T


def gather_call(idx, n_dev, c_parts, r_parts):
    tok, rank = c_parts[0].shape
    d_r = r_parts[0].shape[0]
    seq = n_dev * tok
    whole = lambda shape: pl.BlockSpec(shape, lambda i, idx: (0, 0))
    shapes = [(seq, rank), (rank, seq), (seq, d_r), (d_r, seq)]
    return pl.pallas_call(
        functools.partial(gather_kernel, n_dev),
        grid_spec=pltpu.PrefetchScalarGridSpec(
            num_scalar_prefetch=1, grid=(1,),
            in_specs=[whole((tok, rank))] * 4 + [whole((d_r, tok))] * 4,
            out_specs=[whole(s) for s in shapes]),
        out_shape=[sds(s, BF16) for s in shapes],
        compiler_params=params(60),
        cost_estimate=pl.CostEstimate(flops=10 ** 9, bytes_accessed=8 * 2 ** 20, transcendentals=0),
        name="gather",
    )(idx, *c_parts, *r_parts)


def relay_kernel(idx_ref, *refs):
    wide_s = refs[-1]
    n = len(refs) // 2
    for in_ref, out_ref in zip(refs[:n], refs[n:-1]):
        heads, rows_n, d = out_ref.shape
        wide_s[...] = in_ref[...].astype(F32).reshape(rows_n * heads, d)
        for h in range(heads):
            out_ref[h] = wide_s[pl.ds(h, rows_n, stride=heads), :].astype(BF16)


def relay_call(idx, w_uk, w_uv, d_out):
    tok, n_heads, d = d_out.shape
    heads = n_heads // 2
    n = 128
    near = pl.BlockSpec((n, heads, d), lambda i, idx: (i, idx[1], 0))
    away = pl.BlockSpec((n, heads, d), lambda i, idx: (i, 1 - idx[1], 0))
    return pl.pallas_call(
        relay_kernel,
        grid_spec=pltpu.PrefetchScalarGridSpec(
            num_scalar_prefetch=1, grid=(tok // n,), in_specs=[away, near, near, near],
            out_specs=[pl.BlockSpec((heads, n, d), lambda i, idx: (0, i, 0))] * 4,
            scratch_shapes=[pltpu.VMEM((n * heads, d), F32)]),
        out_shape=[sds((heads, tok, d), BF16)] * 4,
        compiler_params=params(60),
        cost_estimate=pl.CostEstimate(flops=10 ** 9, bytes_accessed=16 * d_out.size, transcendentals=0),
        name="relay",
    )(idx, d_out, d_out, w_uk, w_uv)


def out_kernel(idx_ref, own_ref, oth_ref, out_ref, wide_s):
    core = idx_ref[1]
    heads, n, d = own_ref.shape
    for side, ref in ((core, own_ref), (1 - core, oth_ref)):
        for h in range(heads):
            wide_s[pl.ds(h, n, stride=heads), :] = ref[h].astype(F32)
        out_ref[:, pl.ds(pl.multiple_of(side * heads, heads), heads), :] = wide_s[...].reshape(n, heads, d).astype(BF16)


def out_call(idx, own, oth):
    heads, tok, d = own.shape
    n = 128
    part = pl.BlockSpec((heads, n, d), lambda i, idx: (0, i, 0))
    return pl.pallas_call(
        out_kernel,
        grid_spec=pltpu.PrefetchScalarGridSpec(
            num_scalar_prefetch=1, grid=(tok // n,), in_specs=[part, part],
            out_specs=pl.BlockSpec((n, 2 * heads, d), lambda i, idx: (i, 0, 0)),
            scratch_shapes=[pltpu.VMEM((n * heads, d), F32)]),
        out_shape=sds((tok, 2 * heads, d), BF16),
        compiler_params=params(60),
        cost_estimate=pl.CostEstimate(flops=10 ** 9, bytes_accessed=4 * own.size * 2, transcendentals=0),
        name="out",
    )(idx, own, oth)


def place_kernel(idx_ref, part_ref, full_ref, out_ref):
    out_ref[...] = part_ref[...]


def place_call(idx, part, full, step):
    n, a, b = part.shape
    return pl.pallas_call(
        place_kernel,
        grid_spec=pltpu.PrefetchScalarGridSpec(
            num_scalar_prefetch=1, grid=(n // step,),
            in_specs=[pl.BlockSpec((step, a, b), lambda h, idx: (h, 0, 0)), pl.BlockSpec(memory_space=pl.ANY)],
            out_specs=pl.BlockSpec((step, a, b), lambda h, idx: ((1 - idx[1]) * (n // step) + h, 0, 0))),
        out_shape=sds(full.shape, full.dtype),
        input_output_aliases={2: 0},
        compiler_params=params(60),
        cost_estimate=pl.CostEstimate(flops=10 ** 9, bytes_accessed=2 * part.size * part.dtype.itemsize, transcendentals=0),
        name="place",
    )(idx, part, full)


def join_kernel(n_parts, idx_ref, *refs):
    a_refs, b_refs = refs[:n_parts], refs[n_parts:2 * n_parts]
    k_ref, v_ref = refs[-2:]
    d_n = k_ref.shape[2]
    h = 0
    for a_ref, b_ref in zip(a_refs, b_refs):
        for g in range(a_ref.shape[0]):
            s = a_ref[g] + b_ref[g]
            k_ref[:, h, :] = s[:, :d_n]
            v_ref[:, h, :] = s[:, d_n:]
            h += 1


def join_call(block, parts_a, parts_b, carried, n_heads):
    rank, kv = parts_a[0].shape[1:]
    n_parts = len(parts_a)
    heads = sum(p.shape[0] for p in parts_a)
    r_blk = 128
    parts = [pl.BlockSpec((p.shape[0], r_blk, kv), lambda i, idx: (0, i, 0)) for p in parts_a]
    out = pl.BlockSpec((r_blk, heads, kv // 2), lambda i, idx: (i, idx[0], 0))
    args = [block, *parts_a, *parts_b, *carried]
    return pl.pallas_call(
        functools.partial(join_kernel, n_parts),
        grid_spec=pltpu.PrefetchScalarGridSpec(
            num_scalar_prefetch=1, grid=(rank // r_blk,),
            in_specs=parts + parts + [pl.BlockSpec(memory_space=pl.ANY)] * len(carried),
            out_specs=[out, out]),
        out_shape=[sds((rank, n_heads, kv // 2), F32)] * 2,
        input_output_aliases={1 + 2 * n_parts + i: i for i in range(len(carried))},
        compiler_params=params(60),
        cost_estimate=pl.CostEstimate(flops=10 ** 9, bytes_accessed=3 * heads * rank * kv * 4, transcendentals=0),
        name="join",
    )(*args)


def solution(mesh):
    n_cp = mesh.shape['cp']
    n_tp = mesh.shape['tp']
    cp_half = n_cp // 2
    x_perm = [(d, (d + 2) % n_cp) for d in range(n_cp)]
    core_perm = [(d, d ^ 1) for d in range(n_cp)]
    tp_perm = [(d, (d + 1) % n_tp) for d in range(n_tp)]
    seq_spec = P(('dp', 'cp'), None)
    head_spec = P(('dp', 'cp'), 'tp', None)
    weight_spec = P(None, 'tp', None)
    grad_spec = P('dp', 'tp', None)

    def device_fn(c_latent, k_rope, q_heads, d_out, w_uk, w_uv):
        _, rank = c_latent.shape
        n_heads = q_heads.shape[1]
        half_heads = n_heads // 2
        d_r = k_rope.shape[1]
        scale = q_heads.shape[2] ** -0.5
        me = lax.axis_index('cp')
        chip, core = me // 2, me % 2
        my_tp = lax.axis_index('tp')
        swap_x = lambda a: lax.ppermute(a, 'cp', x_perm)
        swap_core = lambda a: lax.ppermute(a, 'cp', core_perm)
        swap_tp = lambda a: lax.ppermute(a, 'tp', tp_perm)

        def parts(own):
            far = swap_x(own)
            return own, swap_core(own), far, swap_core(far)

        idx = jnp.stack([chip, core]).astype(jnp.int32)
        c_all, ct_all, r_all, rt_all = gather_call(idx, n_cp, parts(c_latent), parts(k_rope.T))
        do_send, do_all, w_k, w_v = relay_call(idx, w_uk, w_uv, d_out)
        q_all = q_heads.transpose(1, 2, 0)
        away = (1 - core) * half_heads
        q_oth = swap_core(lax.dynamic_slice_in_dim(q_all, away, half_heads, 0))
        do_oth = swap_core(do_send)

        carried, own, far, near, far_near = (), [], [], [], []
        first = 0
        for count in sum(GROUPS, ()):
            idx_g = jnp.stack([chip, core, jnp.int32(first)]).astype(jnp.int32)
            outs = group_call(count, cp_half, scale, idx_g, c_all, ct_all, r_all, rt_all, w_k, w_v,
                      q_all, q_oth, do_all, do_oth, carried)
            carried = outs[:6]
            own.append(outs[6])
            far.append(swap_x(outs[6]))
            near.append(swap_core(outs[6]))
            far_near.append(swap_core(far[-1]))
            first += count
        o_own, o_oth, dq_full, dq_oth, dkv, dr = carried

        def fold(arr, axis, pos, swap):
            keep = lax.dynamic_index_in_dim(arr, pos, axis, keepdims=False)
            send = lax.dynamic_index_in_dim(arr, 1 - pos, axis, keepdims=False)
            return keep + swap(send)

        full = []
        for part in dc_call(idx, dkv, w_k, w_v, dr):
            part = part.reshape(2, cp_half, 2, PIECE, -1)
            part = fold(part, 0, core, swap_core)
            part = fold(part, 1, my_tp, swap_tp)
            part = fold(part, 0, chip, swap_x)
            mate = swap_tp(part)
            full.append(jnp.where(my_tp == 0, jnp.concatenate([part, mate], axis=0), jnp.concatenate([mate, part], axis=0)))
        dc = jnp.concatenate([full[0], full[1][:, :rank // 2]], axis=1)
        dr_out = full[1][:, rank // 2:rank // 2 + d_r]

        dws, g0 = (), 0
        for i, groups in enumerate(GROUPS):
            sel = slice(g0, g0 + len(groups))
            g0 += len(groups)
            for side, a, b in ((core, own, far), (1 - core, near, far_near)):
                block = (side * len(GROUPS) + i).reshape(1).astype(jnp.int32)
                dws = join_call(block, a[sel], b[sel], dws, n_heads)
        dq = place_call(idx, swap_core(dq_oth), dq_full, 2).transpose(2, 0, 1)
        out = out_call(idx, o_own, swap_core(o_oth))
        return (out, dq, dc, dr_out, *dws)

    return jax.shard_map(device_fn, mesh=mesh,
                         in_specs=(seq_spec, seq_spec, head_spec, head_spec, weight_spec, weight_spec),
                         out_specs=(head_spec, head_spec, seq_spec, seq_spec, grad_spec, grad_spec),
                         check_vma=False)
```

```python
import functools
import math

import jax
import jax.numpy as jnp
from jax import lax
from jax.experimental import pallas as pl
from jax.experimental.pallas import tpu as pltpu
from jax.sharding import PartitionSpec as P


NEG_BIG = -1.0e30
PIECE = 256
GROUPS = ((2, 3, 3), (4, 4))
F32 = jnp.float32
BF16 = jnp.bfloat16


def dot(a, b):
    return jnp.dot(a, b, preferred_element_type=F32)


def dot_t(a, b):
    return lax.dot_general(a, b, (((1,), (1,)), ((), ())), preferred_element_type=F32)


def rows(i, n=1):
    return pl.ds(i * PIECE, n * PIECE)


def params(mib):
    return pltpu.CompilerParams(dimension_semantics=("arbitrary",), vmem_limit_bytes=mib * 2 ** 20)


def head_body(lens, scale, c_ref, ct_ref, w_s, k_s, kt_s, v_s, vt_s, qt_s, do_s, s_s, p_s, ds_s,
              o_s, dqt_s, dw_ref, dkv_ref, dr_ref):
    n_max = max(lens)
    n_rows = n_max * PIECE
    d_n = v_s.shape[1]
    to_log2 = scale * math.log2(math.e)
    for j in range(0, n_max, 2):
        kv = dot(c_ref[rows(j, 2), :], w_s[...]).astype(BF16)
        k_s[rows(j, 2), 0:d_n] = kv[:, :d_n]
        v_s[rows(j, 2), :] = kv[:, d_n:]
        kt_s[0:d_n, rows(j, 2)] = kv[:, :d_n].T
        vt_s[:, rows(j, 2)] = kv[:, d_n:].T
    key_i = lax.broadcasted_iota(jnp.int32, (PIECE, PIECE), 0)
    qry_i = lax.broadcasted_iota(jnp.int32, (PIECE, PIECE), 1)
    tops = {}

    def score(b):
        n, base = lens[b], sum(lens[:b])
        qt_b = qt_s[:, rows(b)]
        top8 = jnp.full((8, PIECE), NEG_BIG, F32)
        for j in range(n):
            s = dot(k_s[rows(j), :], qt_b)
            if j == n - 1:
                s = jnp.where(key_i <= qry_i, s, NEG_BIG)
            s_s[rows(base + j), :] = s
            top8 = jnp.maximum(top8, jnp.max(s.reshape(PIECE // 8, 8, PIECE), axis=0))
        tops[b] = jnp.max(top8, axis=0, keepdims=True) * to_log2

    invs = {}

    def soft(b):
        n, base = lens[b], sum(lens[:b])
        sum8 = jnp.zeros((8, PIECE), F32)
        for j in range(n):
            p = jnp.exp2(s_s[rows(base + j), :] * to_log2 - tops[b])
            sum8 = sum8 + jnp.sum(p.reshape(PIECE // 8, 8, PIECE), axis=0)
            s_s[rows(base + j), :] = p
            p_s[rows(j), rows(b)] = p.astype(BF16)
        invs[b] = 1.0 / jnp.sum(sum8, axis=0, keepdims=True)

    def back(b):
        n, base, inv = lens[b], sum(lens[:b]), invs[b]
        do_t = do_s[rows(b), :].T
        o_t = dot(vt_s[:, 0:n * PIECE], p_s[0:n * PIECE, rows(b)]) * inv
        o_s[rows(b), :] = o_t.T.astype(BF16)
        d_dot = jnp.sum(o_t * do_t.astype(F32), axis=0, keepdims=True)
        for j in range(n):
            dp = dot(v_s[rows(j), :], do_t)
            p = s_s[rows(base + j), :] * inv
            p_s[rows(j), rows(b)] = p.astype(BF16)
            ds_s[rows(j), rows(b)] = (p * (dp - d_dot)).astype(BF16)
        dqt_s[:, rows(b)] = dot(kt_s[:, 0:n * PIECE], ds_s[0:n * PIECE, rows(b)]) * scale

    score(0)
    for b in range(4):
        soft(b)
        if b < 3:
            score(b + 1)
        back(b)
    edges = sorted({0, *lens})
    for j, j_end in zip(edges[:-1], edges[1:]):
        w = PIECE * sum(1 for n in lens if n > j)
        at = rows(j, j_end - j)
        dv = dot(p_s[at, 0:w], do_s[0:w, :])
        dk = dot_t(ds_s[at, 0:w], qt_s[:, 0:w]) * scale
        dkv_ref[at, 0:d_n] = dk[:, :d_n].astype(BF16)
        dkv_ref[at, d_n:] = dv.astype(BF16)
        dr_ref[at, :] += dk[:, d_n:]
    if n_rows < dkv_ref.shape[0]:
        dkv_ref[n_rows:, :] = jnp.zeros((dkv_ref.shape[0] - n_rows, dkv_ref.shape[1]), BF16)
    for i in range(2):
        dw_ref[0, rows(i), :] = dot(ct_ref[rows(i), 0:n_rows], dkv_ref[0:n_rows, :])


def group_kernel(cp_half, scale, n_alias, idx_ref, c_ref, ct_ref, r_ref, rt_ref, wk_ref, wv_ref, q_own, q_oth, do_own, do_oth, *rest):
    (o_own, o_oth, dq_own, dq_oth, dkv_ref, dr_ref, dw_ref,
     w_s, k_s, kt_s, v_s, vt_s, qt_s, do_s, s_s, p_s, ds_s, o_s, dqt_s) = rest[n_alias:]
    d_n = v_s.shape[1]
    core = idx_ref[1]

    @pl.when(pl.program_id(0) == 0)
    def _():
        k_s[:, d_n:] = r_ref[...]
        kt_s[d_n:, :] = rt_ref[...]
        dr_ref[...] = rest[n_alias - 1][...] if n_alias else jnp.zeros(dr_ref.shape, F32)

    w_s[:, 0:d_n] = wk_ref[0]
    w_s[:, d_n:] = wv_ref[0]

    def at(i):
        return pl.ds(pl.multiple_of(i * PIECE, PIECE), PIECE)

    own_hi, own_lo, oth_hi, oth_lo = core, 3 - core, 1 - core, 2 + core
    lo, hi = pl.ds(0, PIECE), pl.ds(PIECE, PIECE)
    for pos, half, q_ref, do_ref in ((own_lo, lo, q_own, do_own), (own_hi, hi, q_own, do_own),
                                     (oth_lo, lo, q_oth, do_oth), (oth_hi, hi, q_oth, do_oth)):
        qt_s[:, at(pos)] = q_ref[0, :, half]
        do_s[at(pos), :] = do_ref[0, half, :]
    n_pieces = 4 * cp_half
    for chip in range(cp_half):
        dev_a, dev_b = 2 * chip, 2 * chip + 1
        lens = (n_pieces - dev_a, n_pieces - dev_b, dev_b + 1, dev_a + 1)
        pl.when(idx_ref[0] == chip)(functools.partial(
            head_body, lens, scale, c_ref, ct_ref, w_s, k_s, kt_s, v_s, vt_s, qt_s, do_s, s_s, p_s, ds_s,
            o_s, dqt_s, dw_ref, dkv_ref, dr_ref))
    for pos, half, o_ref, dq_ref in ((own_lo, lo, o_own, dq_own), (own_hi, hi, o_own, dq_own),
                                     (oth_lo, lo, o_oth, dq_oth), (oth_hi, hi, o_oth, dq_oth)):
        o_ref[0, half, :] = o_s[at(pos), :]
        dq_ref[0, :, half] = dqt_s[:, at(pos)]


sds = jax.ShapeDtypeStruct


def group_call(count, cp_half, scale, idx, c_all, ct_all, r_all, rt_all, w_k, w_v, q_all, q_oth, do_all, do_oth, carried):
    seq, rank = c_all.shape
    d_r = r_all.shape[1]
    half_heads, d_qk, tok = q_oth.shape
    d_v = do_oth.shape[2]
    kv = w_k.shape[2] + w_v.shape[2]
    whole = lambda *shape: pl.BlockSpec(shape, lambda h, idx: (0,) * len(shape), pipeline_mode=pl.Buffered(1))
    mine = lambda *shape: pl.BlockSpec((1,) + shape, lambda h, idx: (idx[1] * half_heads + idx[2] + h, 0, 0))
    part = lambda *shape: pl.BlockSpec((1,) + shape, lambda h, idx: (idx[2] + h, 0, 0))
    in_specs = [whole(seq, rank), whole(rank, seq), whole(seq, d_r), whole(d_r, seq),
                part(rank, w_k.shape[2]), part(rank, d_v), mine(d_qk, tok), part(d_qk, tok), part(tok, d_v), part(tok, d_v)]
    out_specs = [part(tok, d_v), part(tok, d_v), mine(d_qk, tok), part(d_qk, tok),
                 pl.BlockSpec((seq, kv), lambda h, idx: (0, idx[2] + h)),
                 pl.BlockSpec((seq, d_r), lambda h, idx: (0, 0)),
                 pl.BlockSpec((1, rank, kv), lambda h, idx: (h, 0, 0))]
    out_shape = [sds((half_heads, tok, d_v), BF16), sds((half_heads, tok, d_v), BF16),
                 sds((2 * half_heads, d_qk, tok), F32), sds((half_heads, d_qk, tok), F32),
                 sds((seq, half_heads * kv), BF16), sds((seq, d_r), F32), sds((count, rank, kv), F32)]
    args = [idx, c_all, ct_all, r_all, rt_all, w_k, w_v, q_all, q_oth, do_all, do_oth]
    aliases = {}
    for i, arr in enumerate(carried):
        aliases[len(args)] = i
        args.append(arr)
        in_specs.append(pl.BlockSpec(memory_space=pl.ANY))
    if carried:
        in_specs[-1] = whole(seq, d_r)
    pairs = 2 * tok * (seq // 2 + PIECE // 2)
    flops = count * (2 * pairs * (3 * d_qk + 3 * d_v) + 6 * seq * rank * kv)
    return pl.pallas_call(
        functools.partial(group_kernel, cp_half, scale, len(carried)),
        grid_spec=pltpu.PrefetchScalarGridSpec(
            num_scalar_prefetch=1, grid=(count,), in_specs=in_specs, out_specs=out_specs,
            scratch_shapes=[
                pltpu.VMEM((rank, kv), BF16),
                pltpu.VMEM((seq, d_qk), BF16), pltpu.VMEM((d_qk, seq), BF16),
                pltpu.VMEM((seq, d_v), BF16), pltpu.VMEM((d_v, seq), BF16),
                pltpu.VMEM((d_qk, 2 * tok), BF16), pltpu.VMEM((2 * tok, d_v), BF16),
                pltpu.VMEM((seq * 2 + 2 * PIECE, PIECE), F32),
                pltpu.VMEM((seq, 2 * tok), BF16), pltpu.VMEM((seq, 2 * tok), BF16),
                pltpu.VMEM((2 * tok, d_v), BF16), pltpu.VMEM((d_qk, 2 * tok), F32)]),
        out_shape=out_shape,
        input_output_aliases=aliases,
        compiler_params=params(60),
        cost_estimate=pl.CostEstimate(flops=int(flops), bytes_accessed=count * 4 * 2 ** 20, transcendentals=count * pairs),
        name="heads",
    )(*args)


def dc_kernel(idx_ref, lo_ref, hi_ref, wk_ref, wv_ref, dr_lo, dr_hi, *refs):
    sends, keeps, w_s = refs[0:2], refs[2:4], refs[4]
    heads, _, d_n = wk_ref.shape
    i = pl.program_id(0)

    @pl.when(i == 0)
    def _():
        for g in range(heads):
            w_s[:, 2 * g * d_n:(2 * g + 1) * d_n] = wk_ref[g]
            w_s[:, (2 * g + 1) * d_n:(2 * g + 2) * d_n] = wv_ref[g]

    def fill(outs):
        for j, ref in enumerate(outs):
            for k, (dkv_ref, dr_ref) in enumerate(((lo_ref, dr_lo), (hi_ref, dr_hi))):
                ref[0, k, :, 0:PIECE] = dot_t(dkv_ref[...], w_s[rows(j), :])
                if j == 1:
                    dr = dr_ref[...]
                    ref[0, k, :, PIECE:] = jnp.concatenate([dr, jnp.zeros_like(dr)], axis=1)

    pl.when(i < 2)(functools.partial(fill, sends))
    pl.when(i >= 2)(functools.partial(fill, keeps))


def dc_call(idx, dkv, w_k, w_v, dr):
    seq, d_r = dr.shape
    half_heads, rank, d_n = w_k.shape
    kv = d_n + w_v.shape[2]
    n = seq // (2 * PIECE)
    dev = lambda i, idx: 2 * (i % 2) + jnp.where(i < 2, 1 - idx[1], idx[1])
    lo = lambda w: pl.BlockSpec((PIECE, w), lambda i, idx: (dev(i, idx), 0))
    hi = lambda w: pl.BlockSpec((PIECE, w), lambda i, idx: (2 * n - 1 - dev(i, idx), 0))
    w_spec = pl.BlockSpec((half_heads, rank, d_n), lambda i, idx: (0, 0, 0), pipeline_mode=pl.Buffered(1))
    shapes = [(n // 2, 2, PIECE, rank // 2), (n // 2, 2, PIECE, rank // 2 + 2 * d_r)] * 2
    maps = [lambda i, idx: (jnp.minimum(i, 1), 0, 0, 0)] * 2 + [lambda i, idx: (jnp.maximum(i - 2, 0), 0, 0, 0)] * 2
    return pl.pallas_call(
        dc_kernel,
        grid_spec=pltpu.PrefetchScalarGridSpec(
            num_scalar_prefetch=1, grid=(n,),
            in_specs=[lo(half_heads * kv), hi(half_heads * kv), w_spec, w_spec, lo(d_r), hi(d_r)],
            out_specs=[pl.BlockSpec((1,) + s[1:], m) for s, m in zip(shapes, maps)],
            scratch_shapes=[pltpu.VMEM((rank, half_heads * kv), BF16)]),
        out_shape=[sds(s, F32) for s in shapes],
        compiler_params=params(60),
        cost_estimate=pl.CostEstimate(flops=2 * seq * rank * kv * half_heads, bytes_accessed=30 * 2 ** 20, transcendentals=0),
        name="dc",
    )(idx, dkv, dkv, w_k, w_v, dr, dr)


def gather_kernel(n_dev, idx_ref, *refs):
    c_refs, r_refs = refs[0:4], refs[4:8]
    c_all, ct_all, r_all, rt_all = refs[8:]
    chip, core = idx_ref[0], idx_ref[1]
    devs = (2 * chip + core, 2 * chip + 1 - core, 2 - 2 * chip + core, 3 - 2 * chip - core)
    for dev, c_ref, r_ref in zip(devs, c_refs, r_refs):
        for piece, half in ((dev, rows(0)), (2 * n_dev - 1 - dev, rows(1))):
            at = pl.ds(pl.multiple_of(piece * PIECE, PIECE), PIECE)
            c = c_ref[half, :]
            c_all[at, :] = c
            ct_all[:, at] = c.T
            r = r_ref[:, half]
            rt_all[:, at] = r
            r_all[at, :] = r.T


def gather_call(idx, n_dev, c_parts, r_parts):
    tok, rank = c_parts[0].shape
    d_r = r_parts[0].shape[0]
    seq = n_dev * tok
    whole = lambda shape: pl.BlockSpec(shape, lambda i, idx: (0, 0))
    shapes = [(seq, rank), (rank, seq), (seq, d_r), (d_r, seq)]
    return pl.pallas_call(
        functools.partial(gather_kernel, n_dev),
        grid_spec=pltpu.PrefetchScalarGridSpec(
            num_scalar_prefetch=1, grid=(1,),
            in_specs=[whole((tok, rank))] * 4 + [whole((d_r, tok))] * 4,
            out_specs=[whole(s) for s in shapes]),
        out_shape=[sds(s, BF16) for s in shapes],
        compiler_params=params(60),
        cost_estimate=pl.CostEstimate(flops=10 ** 9, bytes_accessed=8 * 2 ** 20, transcendentals=0),
        name="gather",
    )(idx, *c_parts, *r_parts)


def relay_kernel(idx_ref, *refs):
    wide_s = refs[-1]
    n = len(refs) // 2
    for in_ref, out_ref in zip(refs[:n], refs[n:-1]):
        heads, rows_n, d = out_ref.shape
        wide_s[...] = in_ref[...].astype(F32).reshape(rows_n * heads, d)
        for h in range(heads):
            out_ref[h] = wide_s[pl.ds(h, rows_n, stride=heads), :].astype(BF16)


def relay_call(idx, w_uk, w_uv, d_out):
    tok, n_heads, d = d_out.shape
    heads = n_heads // 2
    n = 128
    near = pl.BlockSpec((n, heads, d), lambda i, idx: (i, idx[1], 0))
    away = pl.BlockSpec((n, heads, d), lambda i, idx: (i, 1 - idx[1], 0))
    return pl.pallas_call(
        relay_kernel,
        grid_spec=pltpu.PrefetchScalarGridSpec(
            num_scalar_prefetch=1, grid=(tok // n,), in_specs=[away, near, near, near],
            out_specs=[pl.BlockSpec((heads, n, d), lambda i, idx: (0, i, 0))] * 4,
            scratch_shapes=[pltpu.VMEM((n * heads, d), F32)]),
        out_shape=[sds((heads, tok, d), BF16)] * 4,
        compiler_params=params(60),
        cost_estimate=pl.CostEstimate(flops=10 ** 9, bytes_accessed=16 * d_out.size, transcendentals=0),
        name="relay",
    )(idx, d_out, d_out, w_uk, w_uv)


def out_kernel(idx_ref, own_ref, oth_ref, out_ref, wide_s):
    core = idx_ref[1]
    heads, n, d = own_ref.shape
    for side, ref in ((core, own_ref), (1 - core, oth_ref)):
        for h in range(heads):
            wide_s[pl.ds(h, n, stride=heads), :] = ref[h].astype(F32)
        out_ref[:, pl.ds(pl.multiple_of(side * heads, heads), heads), :] = wide_s[...].reshape(n, heads, d).astype(BF16)


def out_call(idx, own, oth):
    heads, tok, d = own.shape
    n = 128
    part = pl.BlockSpec((heads, n, d), lambda i, idx: (0, i, 0))
    return pl.pallas_call(
        out_kernel,
        grid_spec=pltpu.PrefetchScalarGridSpec(
            num_scalar_prefetch=1, grid=(tok // n,), in_specs=[part, part],
            out_specs=pl.BlockSpec((n, 2 * heads, d), lambda i, idx: (i, 0, 0)),
            scratch_shapes=[pltpu.VMEM((n * heads, d), F32)]),
        out_shape=sds((tok, 2 * heads, d), BF16),
        compiler_params=params(60),
        cost_estimate=pl.CostEstimate(flops=10 ** 9, bytes_accessed=4 * own.size * 2, transcendentals=0),
        name="out",
    )(idx, own, oth)


def place_kernel(idx_ref, part_ref, full_ref, out_ref):
    out_ref[...] = part_ref[...]


def place_call(idx, part, full, step):
    n, a, b = part.shape
    return pl.pallas_call(
        place_kernel,
        grid_spec=pltpu.PrefetchScalarGridSpec(
            num_scalar_prefetch=1, grid=(n // step,),
            in_specs=[pl.BlockSpec((step, a, b), lambda h, idx: (h, 0, 0)), pl.BlockSpec(memory_space=pl.ANY)],
            out_specs=pl.BlockSpec((step, a, b), lambda h, idx: ((1 - idx[1]) * (n // step) + h, 0, 0))),
        out_shape=sds(full.shape, full.dtype),
        input_output_aliases={2: 0},
        compiler_params=params(60),
        cost_estimate=pl.CostEstimate(flops=10 ** 9, bytes_accessed=2 * part.size * part.dtype.itemsize, transcendentals=0),
        name="place",
    )(idx, part, full)


def join_kernel(n_parts, idx_ref, *refs):
    a_refs, b_refs = refs[:n_parts], refs[n_parts:2 * n_parts]
    k_ref, v_ref = refs[-2:]
    d_n = k_ref.shape[2]
    h = 0
    for a_ref, b_ref in zip(a_refs, b_refs):
        for g in range(a_ref.shape[0]):
            s = a_ref[g] + b_ref[g]
            k_ref[:, h, :] = s[:, :d_n]
            v_ref[:, h, :] = s[:, d_n:]
            h += 1


def join_call(block, parts_a, parts_b, carried, n_heads):
    rank, kv = parts_a[0].shape[1:]
    n_parts = len(parts_a)
    heads = sum(p.shape[0] for p in parts_a)
    r_blk = 128
    parts = [pl.BlockSpec((p.shape[0], r_blk, kv), lambda i, idx: (0, i, 0)) for p in parts_a]
    out = pl.BlockSpec((r_blk, heads, kv // 2), lambda i, idx: (i, idx[0], 0))
    args = [block, *parts_a, *parts_b, *carried]
    return pl.pallas_call(
        functools.partial(join_kernel, n_parts),
        grid_spec=pltpu.PrefetchScalarGridSpec(
            num_scalar_prefetch=1, grid=(rank // r_blk,),
            in_specs=parts + parts + [pl.BlockSpec(memory_space=pl.ANY)] * len(carried),
            out_specs=[out, out]),
        out_shape=[sds((rank, n_heads, kv // 2), F32)] * 2,
        input_output_aliases={1 + 2 * n_parts + i: i for i in range(len(carried))},
        compiler_params=params(60),
        cost_estimate=pl.CostEstimate(flops=10 ** 9, bytes_accessed=3 * heads * rank * kv * 4, transcendentals=0),
        name="join",
    )(*args)


def solution(mesh):
    n_cp = mesh.shape['cp']
    n_tp = mesh.shape['tp']
    cp_half = n_cp // 2
    x_perm = [(d, (d + 2) % n_cp) for d in range(n_cp)]
    core_perm = [(d, d ^ 1) for d in range(n_cp)]
    tp_perm = [(d, (d + 1) % n_tp) for d in range(n_tp)]
    seq_spec = P(('dp', 'cp'), None)
    head_spec = P(('dp', 'cp'), 'tp', None)
    weight_spec = P(None, 'tp', None)
    grad_spec = P('dp', 'tp', None)

    def device_fn(c_latent, k_rope, q_heads, d_out, w_uk, w_uv):
        _, rank = c_latent.shape
        n_heads = q_heads.shape[1]
        half_heads = n_heads // 2
        d_r = k_rope.shape[1]
        scale = q_heads.shape[2] ** -0.5
        me = lax.axis_index('cp')
        chip, core = me // 2, me % 2
        my_tp = lax.axis_index('tp')
        swap_x = lambda a: lax.ppermute(a, 'cp', x_perm)
        swap_core = lambda a: lax.ppermute(a, 'cp', core_perm)
        swap_tp = lambda a: lax.ppermute(a, 'tp', tp_perm)

        def parts(own):
            far = swap_x(own)
            return own, swap_core(own), far, swap_core(far)

        idx = jnp.stack([chip, core]).astype(jnp.int32)
        c_all, ct_all, r_all, rt_all = gather_call(idx, n_cp, parts(c_latent), parts(k_rope.T))
        do_send, do_all, w_k, w_v = relay_call(idx, w_uk, w_uv, d_out)
        q_all = q_heads.transpose(1, 2, 0)
        away = (1 - core) * half_heads
        q_oth = swap_core(lax.dynamic_slice_in_dim(q_all, away, half_heads, 0))
        do_oth = swap_core(do_send)

        carried, own, far, near, far_near = (), [], [], [], []
        first = 0
        for count in sum(GROUPS, ()):
            idx_g = jnp.stack([chip, core, jnp.int32(first)]).astype(jnp.int32)
            outs = group_call(count, cp_half, scale, idx_g, c_all, ct_all, r_all, rt_all, w_k, w_v,
                      q_all, q_oth, do_all, do_oth, carried)
            carried = outs[:6]
            own.append(outs[6])
            far.append(swap_x(outs[6]))
            near.append(swap_core(outs[6]))
            far_near.append(swap_core(far[-1]))
            first += count
        o_own, o_oth, dq_full, dq_oth, dkv, dr = carried

        def fold(arrs, axis, pos, swap):
            cut = lambda p: [lax.dynamic_index_in_dim(a, p, axis, keepdims=False) for a in arrs]
            return cut(pos) + [swap(functools.reduce(jnp.add, cut(1 - pos)))]

        full = []
        dc_out = dc_call(idx, dkv, w_k, w_v, dr)
        for half in range(2):
            arrs = [dc_out[2 + half], swap_core(dc_out[half])]
            arrs = fold(arrs, 1, my_tp, swap_tp)
            part = functools.reduce(jnp.add, fold(arrs, 0, chip, swap_x))
            mate = swap_tp(part)
            full.append(jnp.where(my_tp == 0, jnp.concatenate([part, mate], axis=0), jnp.concatenate([mate, part], axis=0)))
        dc = jnp.concatenate([full[0], full[1][:, :rank // 2]], axis=1)
        dr_out = full[1][:, rank // 2:rank // 2 + d_r]

        dws, g0 = (), 0
        for i, groups in enumerate(GROUPS):
            sel = slice(g0, g0 + len(groups))
            g0 += len(groups)
            for side, a, b in ((core, own, far), (1 - core, near, far_near)):
                block = (side * len(GROUPS) + i).reshape(1).astype(jnp.int32)
                dws = join_call(block, a[sel], b[sel], dws, n_heads)
        dq = place_call(idx, swap_core(dq_oth), dq_full, 2).transpose(2, 0, 1)
        out = out_call(idx, o_own, swap_core(o_oth))
        return (out, dq, dc, dr_out, *dws)

    return jax.shard_map(device_fn, mesh=mesh,
                         in_specs=(seq_spec, seq_spec, head_spec, head_spec, weight_spec, weight_spec),
                         out_specs=(head_spec, head_spec, seq_spec, seq_spec, grad_spec, grad_spec),
                         check_vma=False)
```

```python
import functools
import math

import jax
import jax.numpy as jnp
from jax import lax
from jax.experimental import pallas as pl
from jax.experimental.pallas import tpu as pltpu
from jax.sharding import PartitionSpec as P


NEG_BIG = -1.0e30
PIECE = 256
GROUPS = ((2, 3, 3), (4, 4))
F32 = jnp.float32
BF16 = jnp.bfloat16


def dot(a, b):
    return jnp.dot(a, b, preferred_element_type=F32)


def dot_t(a, b):
    return lax.dot_general(a, b, (((1,), (1,)), ((), ())), preferred_element_type=F32)


def rows(i, n=1):
    return pl.ds(i * PIECE, n * PIECE)


def params(mib):
    return pltpu.CompilerParams(dimension_semantics=("arbitrary",), vmem_limit_bytes=mib * 2 ** 20)


def head_body(lens, scale, c_ref, ct_ref, w_s, k_s, kt_s, v_s, vt_s, qt_s, do_s, s_s, p_s, ds_s,
              o_s, dqt_s, dw_ref, dkv_ref, dr_ref):
    n_max = max(lens)
    n_rows = n_max * PIECE
    d_n = v_s.shape[1]
    to_log2 = scale * math.log2(math.e)
    for j in range(0, n_max, 2):
        kv = dot(c_ref[rows(j, 2), :], w_s[...]).astype(BF16)
        k_s[rows(j, 2), 0:d_n] = kv[:, :d_n]
        v_s[rows(j, 2), :] = kv[:, d_n:]
        kt_s[0:d_n, rows(j, 2)] = kv[:, :d_n].T
        vt_s[:, rows(j, 2)] = kv[:, d_n:].T
    key_i = lax.broadcasted_iota(jnp.int32, (PIECE, PIECE), 0)
    qry_i = lax.broadcasted_iota(jnp.int32, (PIECE, PIECE), 1)
    tops = {}

    def score(b):
        n, base = lens[b], sum(lens[:b])
        qt_b = qt_s[:, rows(b)]
        top8 = jnp.full((8, PIECE), NEG_BIG, F32)
        for j in range(n):
            s = dot(k_s[rows(j), :], qt_b)
            if j == n - 1:
                s = jnp.where(key_i <= qry_i, s, NEG_BIG)
            s_s[rows(base + j), :] = s
            top8 = jnp.maximum(top8, jnp.max(s.reshape(PIECE // 8, 8, PIECE), axis=0))
        tops[b] = jnp.max(top8, axis=0, keepdims=True) * to_log2

    invs = {}

    def soft(b):
        n, base = lens[b], sum(lens[:b])
        sum8 = jnp.zeros((8, PIECE), F32)
        for j in range(n):
            p = jnp.exp2(s_s[rows(base + j), :] * to_log2 - tops[b])
            sum8 = sum8 + jnp.sum(p.reshape(PIECE // 8, 8, PIECE), axis=0)
            s_s[rows(base + j), :] = p
            p_s[rows(j), rows(b)] = p.astype(BF16)
        invs[b] = 1.0 / jnp.sum(sum8, axis=0, keepdims=True)

    def back(b):
        n, base, inv = lens[b], sum(lens[:b]), invs[b]
        do_t = do_s[rows(b), :].T
        o_t = dot(vt_s[:, 0:n * PIECE], p_s[0:n * PIECE, rows(b)]) * inv
        o_s[rows(b), :] = o_t.T.astype(BF16)
        d_dot = jnp.sum(o_t * do_t.astype(F32), axis=0, keepdims=True)
        for j in range(n):
            dp = dot(v_s[rows(j), :], do_t)
            p = s_s[rows(base + j), :] * inv
            p_s[rows(j), rows(b)] = p.astype(BF16)
            ds_s[rows(j), rows(b)] = (p * (dp - d_dot)).astype(BF16)
        dqt_s[:, rows(b)] = dot(kt_s[:, 0:n * PIECE], ds_s[0:n * PIECE, rows(b)]) * scale

    score(0)
    for b in range(4):
        soft(b)
        if b < 3:
            score(b + 1)
        back(b)
    edges = sorted({0, *lens})
    for j, j_end in zip(edges[:-1], edges[1:]):
        w = PIECE * sum(1 for n in lens if n > j)
        at = rows(j, j_end - j)
        dv = dot(p_s[at, 0:w], do_s[0:w, :])
        dk = dot_t(ds_s[at, 0:w], qt_s[:, 0:w]) * scale
        dkv_ref[at, 0:d_n] = dk[:, :d_n].astype(BF16)
        dkv_ref[at, d_n:] = dv.astype(BF16)
        dr_ref[at, :] += dk[:, d_n:]
    if n_rows < dkv_ref.shape[0]:
        dkv_ref[n_rows:, :] = jnp.zeros((dkv_ref.shape[0] - n_rows, dkv_ref.shape[1]), BF16)
    for i in range(2):
        dw_ref[0, rows(i), :] = dot(ct_ref[rows(i), 0:n_rows], dkv_ref[0:n_rows, :])


def group_kernel(cp_half, scale, n_alias, idx_ref, c_ref, ct_ref, r_ref, rt_ref, wk_ref, wv_ref, q_own, q_oth, do_own, do_oth, *rest):
    (o_own, o_oth, dq_own, dq_oth, dkv_ref, dr_ref, dw_ref,
     w_s, k_s, kt_s, v_s, vt_s, qt_s, do_s, s_s, p_s, ds_s, o_s, dqt_s) = rest[n_alias:]
    d_n = v_s.shape[1]
    core = idx_ref[1]

    @pl.when(pl.program_id(0) == 0)
    def _():
        k_s[:, d_n:] = r_ref[...]
        kt_s[d_n:, :] = rt_ref[...]
        dr_ref[...] = rest[n_alias - 1][...] if n_alias else jnp.zeros(dr_ref.shape, F32)

    w_s[:, 0:d_n] = wk_ref[0]
    w_s[:, d_n:] = wv_ref[0]

    def at(i):
        return pl.ds(pl.multiple_of(i * PIECE, PIECE), PIECE)

    own_hi, own_lo, oth_hi, oth_lo = core, 3 - core, 1 - core, 2 + core
    lo, hi = pl.ds(0, PIECE), pl.ds(PIECE, PIECE)
    for pos, half, q_ref, do_ref in ((own_lo, lo, q_own, do_own), (own_hi, hi, q_own, do_own),
                                     (oth_lo, lo, q_oth, do_oth), (oth_hi, hi, q_oth, do_oth)):
        qt_s[:, at(pos)] = q_ref[0, :, half]
        do_s[at(pos), :] = do_ref[0, half, :]
    n_pieces = 4 * cp_half
    for chip in range(cp_half):
        dev_a, dev_b = 2 * chip, 2 * chip + 1
        lens = (n_pieces - dev_a, n_pieces - dev_b, dev_b + 1, dev_a + 1)
        pl.when(idx_ref[0] == chip)(functools.partial(
            head_body, lens, scale, c_ref, ct_ref, w_s, k_s, kt_s, v_s, vt_s, qt_s, do_s, s_s, p_s, ds_s,
            o_s, dqt_s, dw_ref, dkv_ref, dr_ref))
    for pos, half, o_ref, dq_ref in ((own_lo, lo, o_own, dq_own), (own_hi, hi, o_own, dq_own),
                                     (oth_lo, lo, o_oth, dq_oth), (oth_hi, hi, o_oth, dq_oth)):
        o_ref[0, half, :] = o_s[at(pos), :]
        dq_ref[0, :, half] = dqt_s[:, at(pos)]


sds = jax.ShapeDtypeStruct


def group_call(first, count, cp_half, scale, idx, c_all, ct_all, r_all, rt_all, w_k, w_v, q_all, q_oth, do_all, do_oth, carried):
    seq, rank = c_all.shape
    d_r = r_all.shape[1]
    half_heads, d_qk, tok = q_oth.shape
    d_v = do_oth.shape[2]
    kv = w_k.shape[2] + w_v.shape[2]
    whole = lambda *shape: pl.BlockSpec(shape, lambda h, idx: (0,) * len(shape), pipeline_mode=pl.Buffered(1))
    mine = lambda *shape: pl.BlockSpec((1,) + shape, lambda h, idx: (idx[1] * half_heads + first + h, 0, 0))
    part = lambda *shape: pl.BlockSpec((1,) + shape, lambda h, idx: (first + h, 0, 0))
    in_specs = [whole(seq, rank), whole(rank, seq), whole(seq, d_r), whole(d_r, seq),
                part(rank, w_k.shape[2]), part(rank, d_v), mine(d_qk, tok), part(d_qk, tok), part(tok, d_v), part(tok, d_v)]
    out_specs = [part(tok, d_v), part(tok, d_v), mine(d_qk, tok), part(d_qk, tok),
                 pl.BlockSpec((seq, kv), lambda h, idx: (0, first + h)),
                 pl.BlockSpec((seq, d_r), lambda h, idx: (0, 0)),
                 pl.BlockSpec((1, rank, kv), lambda h, idx: (h, 0, 0))]
    out_shape = [sds((half_heads, tok, d_v), BF16), sds((half_heads, tok, d_v), BF16),
                 sds((2 * half_heads, d_qk, tok), F32), sds((half_heads, d_qk, tok), F32),
                 sds((seq, half_heads * kv), BF16), sds((seq, d_r), F32), sds((count, rank, kv), F32)]
    args = [idx, c_all, ct_all, r_all, rt_all, w_k, w_v, q_all, q_oth, do_all, do_oth]
    aliases = {}
    for i, arr in enumerate(carried):
        aliases[len(args)] = i
        args.append(arr)
        in_specs.append(pl.BlockSpec(memory_space=pl.ANY))
    if carried:
        in_specs[-1] = whole(seq, d_r)
    pairs = 2 * tok * (seq // 2 + PIECE // 2)
    flops = count * (2 * pairs * (3 * d_qk + 3 * d_v) + 6 * seq * rank * kv)
    return pl.pallas_call(
        functools.partial(group_kernel, cp_half, scale, len(carried)),
        grid_spec=pltpu.PrefetchScalarGridSpec(
            num_scalar_prefetch=1, grid=(count,), in_specs=in_specs, out_specs=out_specs,
            scratch_shapes=[
                pltpu.VMEM((rank, kv), BF16),
                pltpu.VMEM((seq, d_qk), BF16), pltpu.VMEM((d_qk, seq), BF16),
                pltpu.VMEM((seq, d_v), BF16), pltpu.VMEM((d_v, seq), BF16),
                pltpu.VMEM((d_qk, 2 * tok), BF16), pltpu.VMEM((2 * tok, d_v), BF16),
                pltpu.VMEM((seq * 2 + 2 * PIECE, PIECE), F32),
                pltpu.VMEM((seq, 2 * tok), BF16), pltpu.VMEM((seq, 2 * tok), BF16),
                pltpu.VMEM((2 * tok, d_v), BF16), pltpu.VMEM((d_qk, 2 * tok), F32)]),
        out_shape=out_shape,
        input_output_aliases=aliases,
        compiler_params=params(60),
        cost_estimate=pl.CostEstimate(flops=int(flops), bytes_accessed=count * 4 * 2 ** 20, transcendentals=count * pairs),
        name="heads",
    )(*args)


def dc_kernel(idx_ref, lo_ref, hi_ref, wk_ref, wv_ref, dr_lo, dr_hi, *refs):
    sends, keeps, w_s = refs[0:2], refs[2:4], refs[4]
    heads, rank, d_n = wk_ref.shape
    i = pl.program_id(0)

    @pl.when(i == 0)
    def _():
        for g in range(heads):
            w_s[:, 2 * g * d_n:(2 * g + 1) * d_n] = wk_ref[g]
            w_s[:, (2 * g + 1) * d_n:(2 * g + 2) * d_n] = wv_ref[g]

    def fill(outs):
        wide, slim = outs
        split = wide.shape[3]
        for k, (dkv_ref, dr_ref) in enumerate(((lo_ref, dr_lo), (hi_ref, dr_hi))):
            for j in range(0, rank, PIECE):
                dc = dot_t(dkv_ref[...], w_s[j:j + PIECE, :])
                n_wide = min(split - j, PIECE)
                wide[0, k, :, j:j + n_wide] = dc[:, :n_wide]
                if n_wide < PIECE:
                    slim[0, k, :, 0:rank - split] = dc[:, n_wide:]
            dr = dr_ref[...]
            slim[0, k, :, rank - split:] = jnp.concatenate([dr, jnp.zeros_like(dr)], axis=1)

    pl.when(i < 2)(functools.partial(fill, sends))
    pl.when(i >= 2)(functools.partial(fill, keeps))


def dc_call(split, idx, dkv, w_k, w_v, dr):
    seq, d_r = dr.shape
    half_heads, rank, d_n = w_k.shape
    kv = d_n + w_v.shape[2]
    n = seq // (2 * PIECE)
    dev = lambda i, idx: 2 * (i % 2) + jnp.where(i < 2, 1 - idx[1], idx[1])
    lo = lambda w: pl.BlockSpec((PIECE, w), lambda i, idx: (dev(i, idx), 0))
    hi = lambda w: pl.BlockSpec((PIECE, w), lambda i, idx: (2 * n - 1 - dev(i, idx), 0))
    w_spec = pl.BlockSpec((half_heads, rank, d_n), lambda i, idx: (0, 0, 0), pipeline_mode=pl.Buffered(1))
    shapes = [(n // 2, 2, PIECE, split), (n // 2, 2, PIECE, rank - split + 2 * d_r)] * 2
    maps = [lambda i, idx: (jnp.minimum(i, 1), 0, 0, 0)] * 2 + [lambda i, idx: (jnp.maximum(i - 2, 0), 0, 0, 0)] * 2
    return pl.pallas_call(
        dc_kernel,
        grid_spec=pltpu.PrefetchScalarGridSpec(
            num_scalar_prefetch=1, grid=(n,),
            in_specs=[lo(half_heads * kv), hi(half_heads * kv), w_spec, w_spec, lo(d_r), hi(d_r)],
            out_specs=[pl.BlockSpec((1,) + s[1:], m) for s, m in zip(shapes, maps)],
            scratch_shapes=[pltpu.VMEM((rank, half_heads * kv), BF16)]),
        out_shape=[sds(s, F32) for s in shapes],
        compiler_params=params(60),
        cost_estimate=pl.CostEstimate(flops=2 * seq * rank * kv * half_heads, bytes_accessed=30 * 2 ** 20, transcendentals=0),
        name="dc",
    )(idx, dkv, dkv, w_k, w_v, dr, dr)


def gather_kernel(n_dev, idx_ref, *refs):
    c_refs, r_refs = refs[0:4], refs[4:8]
    c_all, ct_all, r_all, rt_all = refs[8:]
    chip, core = idx_ref[0], idx_ref[1]
    devs = (2 * chip + core, 2 * chip + 1 - core, 2 - 2 * chip + core, 3 - 2 * chip - core)
    for dev, c_ref, r_ref in zip(devs, c_refs, r_refs):
        for piece, half in ((dev, rows(0)), (2 * n_dev - 1 - dev, rows(1))):
            at = pl.ds(pl.multiple_of(piece * PIECE, PIECE), PIECE)
            c = c_ref[half, :]
            c_all[at, :] = c
            ct_all[:, at] = c.T
            r = r_ref[:, half]
            rt_all[:, at] = r
            r_all[at, :] = r.T


def gather_call(idx, n_dev, c_parts, r_parts):
    tok, rank = c_parts[0].shape
    d_r = r_parts[0].shape[0]
    seq = n_dev * tok
    whole = lambda shape: pl.BlockSpec(shape, lambda i, idx: (0, 0))
    shapes = [(seq, rank), (rank, seq), (seq, d_r), (d_r, seq)]
    return pl.pallas_call(
        functools.partial(gather_kernel, n_dev),
        grid_spec=pltpu.PrefetchScalarGridSpec(
            num_scalar_prefetch=1, grid=(1,),
            in_specs=[whole((tok, rank))] * 4 + [whole((d_r, tok))] * 4,
            out_specs=[whole(s) for s in shapes]),
        out_shape=[sds(s, BF16) for s in shapes],
        compiler_params=params(60),
        cost_estimate=pl.CostEstimate(flops=10 ** 9, bytes_accessed=8 * 2 ** 20, transcendentals=0),
        name="gather",
    )(idx, *c_parts, *r_parts)


def relay_kernel(idx_ref, *refs):
    n = len(refs) // 2
    for in_ref, out_ref in zip(refs[:n], refs[n:]):
        out_ref[...] = jnp.swapaxes(in_ref[...], 0, 1)


def relay_call(idx, w_uk, w_uv, d_out):
    tok, n_heads, d = d_out.shape
    heads = n_heads // 2
    n = 256
    near = pl.BlockSpec((n, heads, d), lambda i, idx: (i, idx[1], 0))
    away = pl.BlockSpec((n, heads, d), lambda i, idx: (i, 1 - idx[1], 0))
    return pl.pallas_call(
        relay_kernel,
        grid_spec=pltpu.PrefetchScalarGridSpec(
            num_scalar_prefetch=1, grid=(tok // n,), in_specs=[away, near, near, near],
            out_specs=[pl.BlockSpec((heads, n, d), lambda i, idx: (0, i, 0))] * 4),
        out_shape=[sds((heads, tok, d), BF16)] * 4,
        compiler_params=params(60),
        cost_estimate=pl.CostEstimate(flops=10 ** 9, bytes_accessed=16 * d_out.size, transcendentals=0),
        name="relay",
    )(idx, d_out, d_out, w_uk, w_uv)


def out_kernel(idx_ref, own_ref, oth_ref, out_ref):
    core = idx_ref[1]
    heads = own_ref.shape[0]
    for side, ref in ((core, own_ref), (1 - core, oth_ref)):
        out_ref[:, pl.ds(pl.multiple_of(side * heads, heads), heads), :] = jnp.swapaxes(ref[...], 0, 1)


def out_call(idx, own, oth):
    heads, tok, d = own.shape
    n = 256
    part = pl.BlockSpec((heads, n, d), lambda i, idx: (0, i, 0))
    return pl.pallas_call(
        out_kernel,
        grid_spec=pltpu.PrefetchScalarGridSpec(
            num_scalar_prefetch=1, grid=(tok // n,), in_specs=[part, part],
            out_specs=pl.BlockSpec((n, 2 * heads, d), lambda i, idx: (i, 0, 0))),
        out_shape=sds((tok, 2 * heads, d), BF16),
        compiler_params=params(60),
        cost_estimate=pl.CostEstimate(flops=10 ** 9, bytes_accessed=4 * own.size * 2, transcendentals=0),
        name="out",
    )(idx, own, oth)


def place_kernel(idx_ref, part_ref, full_ref, out_ref):
    out_ref[...] = part_ref[...]


def place_call(idx, part, full, step):
    n, a, b = part.shape
    return pl.pallas_call(
        place_kernel,
        grid_spec=pltpu.PrefetchScalarGridSpec(
            num_scalar_prefetch=1, grid=(n // step,),
            in_specs=[pl.BlockSpec((step, a, b), lambda h, idx: (h, 0, 0)), pl.BlockSpec(memory_space=pl.ANY)],
            out_specs=pl.BlockSpec((step, a, b), lambda h, idx: ((1 - idx[1]) * (n // step) + h, 0, 0))),
        out_shape=sds(full.shape, full.dtype),
        input_output_aliases={2: 0},
        compiler_params=params(60),
        cost_estimate=pl.CostEstimate(flops=10 ** 9, bytes_accessed=2 * part.size * part.dtype.itemsize, transcendentals=0),
        name="place",
    )(idx, part, full)


def join_kernel(n_parts, idx_ref, *refs):
    a_refs, b_refs = refs[:n_parts], refs[n_parts:2 * n_parts]
    k_ref, v_ref = refs[-2:]
    n_rows, heads, d_n = k_ref.shape
    h = 0
    for a_ref, b_ref in zip(a_refs, b_refs):
        for g in range(a_ref.shape[0]):
            s = a_ref[g] + b_ref[g]
            at = pl.ds(h, n_rows, stride=heads)
            k_ref.reshape(n_rows * heads, d_n)[at, :] = s[:, :d_n]
            v_ref.reshape(n_rows * heads, d_n)[at, :] = s[:, d_n:]
            h += 1


def join_call(idx, block, parts_a, parts_b, carried, n_heads):
    rank, kv = parts_a[0].shape[1:]
    n_parts = len(parts_a)
    heads = sum(p.shape[0] for p in parts_a)
    r_blk = 256
    parts = [pl.BlockSpec((p.shape[0], r_blk, kv), lambda i, idx: (0, i, 0)) for p in parts_a]
    out = pl.BlockSpec((r_blk, heads, kv // 2), lambda i, idx: (i, block(idx[1]), 0))
    args = [idx, *parts_a, *parts_b, *carried]
    return pl.pallas_call(
        functools.partial(join_kernel, n_parts),
        grid_spec=pltpu.PrefetchScalarGridSpec(
            num_scalar_prefetch=1, grid=(rank // r_blk,),
            in_specs=parts + parts + [pl.BlockSpec(memory_space=pl.ANY)] * len(carried),
            out_specs=[out, out]),
        out_shape=[sds((rank, n_heads, kv // 2), F32)] * 2,
        input_output_aliases={1 + 2 * n_parts + i: i for i in range(len(carried))},
        compiler_params=params(60),
        cost_estimate=pl.CostEstimate(flops=10 ** 9, bytes_accessed=3 * heads * rank * kv * 4, transcendentals=0),
        name="join",
    )(*args)


def solution(mesh):
    n_cp = mesh.shape['cp']
    n_tp = mesh.shape['tp']
    cp_half = n_cp // 2
    x_perm = [(d, (d + 2) % n_cp) for d in range(n_cp)]
    core_perm = [(d, d ^ 1) for d in range(n_cp)]
    tp_perm = [(d, (d + 1) % n_tp) for d in range(n_tp)]
    seq_spec = P(('dp', 'cp'), None)
    head_spec = P(('dp', 'cp'), 'tp', None)
    weight_spec = P(None, 'tp', None)
    grad_spec = P('dp', 'tp', None)

    def device_fn(c_latent, k_rope, q_heads, d_out, w_uk, w_uv):
        _, rank = c_latent.shape
        n_heads = q_heads.shape[1]
        half_heads = n_heads // 2
        d_r = k_rope.shape[1]
        d_n = w_uk.shape[2]
        scale = q_heads.shape[2] ** -0.5
        me = lax.axis_index('cp')
        chip, core = me // 2, me % 2
        my_tp = lax.axis_index('tp')
        swap_x = lambda a: lax.ppermute(a, 'cp', x_perm)
        swap_core = lambda a: lax.ppermute(a, 'cp', core_perm)
        swap_tp = lambda a: lax.ppermute(a, 'tp', tp_perm)

        def parts(own):
            far = swap_x(own)
            return own, swap_core(own), far, swap_core(far)

        idx = jnp.stack([chip, core]).astype(jnp.int32)
        c_all, ct_all, r_all, rt_all = gather_call(idx, n_cp, parts(c_latent), parts(k_rope.T))
        do_send, do_all, w_k, w_v = relay_call(idx, w_uk, w_uv, d_out)
        q_all = q_heads.transpose(1, 2, 0)
        away = (1 - core) * half_heads
        q_oth = swap_core(lax.dynamic_slice_in_dim(q_all, away, half_heads, 0))
        do_oth = swap_core(do_send)

        carried, own, far, near, far_near = (), [], [], [], []
        first = 0
        for count in sum(GROUPS, ()):
            outs = group_call(first, count, cp_half, scale, idx, c_all, ct_all, r_all, rt_all, w_k, w_v,
                      q_all, q_oth, do_all, do_oth, carried)
            carried = outs[:6]
            own.append(outs[6])
            far.append(swap_x(outs[6]))
            near.append(swap_core(outs[6]))
            far_near.append(swap_core(far[-1]))
            first += count
        o_own, o_oth, dq_full, dq_oth, dkv, dr = carried

        def fold(arrs, axis, pos, swap):
            cut = lambda p: [lax.dynamic_index_in_dim(a, p, axis, keepdims=False) for a in arrs]
            return cut(pos) + [swap(functools.reduce(jnp.add, cut(1 - pos)))]

        full = []
        split = rank - d_n
        dc_out = dc_call(split, idx, dkv, w_k, w_v, dr)
        for half in range(2):
            arrs = [dc_out[2 + half], swap_core(dc_out[half])]
            arrs = fold(arrs, 1, my_tp, swap_tp)
            part = functools.reduce(jnp.add, fold(arrs, 0, chip, swap_x))
            mate = swap_tp(part)
            full.append(jnp.where(my_tp == 0, jnp.concatenate([part, mate], axis=0), jnp.concatenate([mate, part], axis=0)))
        dc = jnp.concatenate([full[0], full[1][:, :rank - split]], axis=1)
        dr_out = full[1][:, rank - split:rank - split + d_r]

        dws, g0 = (), 0
        for i, groups in enumerate(GROUPS):
            sel = slice(g0, g0 + len(groups))
            g0 += len(groups)
            for s, (a, b) in enumerate(((own, far), (near, far_near))):
                block = lambda c, i=i, s=s: (1 - c if s else c) * len(GROUPS) + i
                dws = join_call(idx, block, a[sel], b[sel], dws, n_heads)
        dq = place_call(idx, swap_core(dq_oth), dq_full, 8).transpose(2, 0, 1)
        out = out_call(idx, o_own, swap_core(o_oth))
        return (out, dq, dc, dr_out, *dws)

    return jax.shard_map(device_fn, mesh=mesh,
                         in_specs=(seq_spec, seq_spec, head_spec, head_spec, weight_spec, weight_spec),
                         out_specs=(head_spec, head_spec, seq_spec, seq_spec, grad_spec, grad_spec),
                         check_vma=False)
```

```python
import functools
import math

import jax
import jax.numpy as jnp
from jax import lax
from jax.experimental import pallas as pl
from jax.experimental.pallas import tpu as pltpu
from jax.sharding import PartitionSpec as P


NEG_BIG = -1.0e30
PIECE = 256
GROUPS = ((2, 2, 2, 2), (4, 4))
F32 = jnp.float32
BF16 = jnp.bfloat16


def dot(a, b):
    return jnp.dot(a, b, preferred_element_type=F32)


def dot_t(a, b):
    return lax.dot_general(a, b, (((1,), (1,)), ((), ())), preferred_element_type=F32)


def rows(i, n=1):
    return pl.ds(i * PIECE, n * PIECE)


def params(mib):
    return pltpu.CompilerParams(dimension_semantics=("arbitrary",), vmem_limit_bytes=mib * 2 ** 20)


def head_body(lens, scale, c_ref, ct_ref, w_s, k_s, kt_s, v_s, vt_s, qt_s, do_s, s_s, p_s, ds_s,
              o_s, dqt_s, dw_ref, dkv_ref, dr_ref):
    n_max = max(lens)
    n_rows = n_max * PIECE
    d_n = v_s.shape[1]
    to_log2 = scale * math.log2(math.e)
    for j in range(0, n_max, 2):
        kv = dot(c_ref[rows(j, 2), :], w_s[...]).astype(BF16)
        k_s[rows(j, 2), 0:d_n] = kv[:, :d_n]
        v_s[rows(j, 2), :] = kv[:, d_n:]
        kt_s[0:d_n, rows(j, 2)] = kv[:, :d_n].T
        vt_s[:, rows(j, 2)] = kv[:, d_n:].T
    key_i = lax.broadcasted_iota(jnp.int32, (PIECE, PIECE), 0)
    qry_i = lax.broadcasted_iota(jnp.int32, (PIECE, PIECE), 1)
    tops = {}

    def score(b):
        n, base = lens[b], sum(lens[:b])
        qt_b = qt_s[:, rows(b)]
        top8 = jnp.full((8, PIECE), NEG_BIG, F32)
        for j in range(n):
            s = dot(k_s[rows(j), :], qt_b)
            if j == n - 1:
                s = jnp.where(key_i <= qry_i, s, NEG_BIG)
            s_s[rows(base + j), :] = s
            top8 = jnp.maximum(top8, jnp.max(s.reshape(PIECE // 8, 8, PIECE), axis=0))
        tops[b] = jnp.max(top8, axis=0, keepdims=True) * to_log2

    invs = {}

    def soft(b):
        n, base = lens[b], sum(lens[:b])
        sum8 = jnp.zeros((8, PIECE), F32)
        for j in range(n):
            p = jnp.exp2(s_s[rows(base + j), :] * to_log2 - tops[b])
            sum8 = sum8 + jnp.sum(p.reshape(PIECE // 8, 8, PIECE), axis=0)
            s_s[rows(base + j), :] = p
            p_s[rows(j), rows(b)] = p.astype(BF16)
        invs[b] = 1.0 / jnp.sum(sum8, axis=0, keepdims=True)

    def back(b):
        n, base, inv = lens[b], sum(lens[:b]), invs[b]
        do_t = do_s[rows(b), :].T
        o_t = dot(vt_s[:, 0:n * PIECE], p_s[0:n * PIECE, rows(b)]) * inv
        o_s[rows(b), :] = o_t.T.astype(BF16)
        d_dot = jnp.sum(o_t * do_t.astype(F32), axis=0, keepdims=True)
        for j in range(n):
            dp = dot(v_s[rows(j), :], do_t)
            p = s_s[rows(base + j), :] * inv
            p_s[rows(j), rows(b)] = p.astype(BF16)
            ds_s[rows(j), rows(b)] = (p * (dp - d_dot)).astype(BF16)
        dqt_s[:, rows(b)] = dot(kt_s[:, 0:n * PIECE], ds_s[0:n * PIECE, rows(b)]) * scale

    score(0)
    for b in range(4):
        soft(b)
        if b < 3:
            score(b + 1)
        back(b)
    edges = sorted({0, *lens})
    for j, j_end in zip(edges[:-1], edges[1:]):
        w = PIECE * sum(1 for n in lens if n > j)
        at = rows(j, j_end - j)
        dv = dot(p_s[at, 0:w], do_s[0:w, :])
        dk = dot_t(ds_s[at, 0:w], qt_s[:, 0:w]) * scale
        dkv_ref[at, 0:d_n] = dk[:, :d_n].astype(BF16)
        dkv_ref[at, d_n:] = dv.astype(BF16)
        dr_ref[at, :] += dk[:, d_n:]
    if n_rows < dkv_ref.shape[0]:
        dkv_ref[n_rows:, :] = jnp.zeros((dkv_ref.shape[0] - n_rows, dkv_ref.shape[1]), BF16)
    for i in range(2):
        dw_ref[0, rows(i), :] = dot(ct_ref[rows(i), 0:n_rows], dkv_ref[0:n_rows, :])


def group_kernel(cp_half, scale, n_alias, idx_ref, c_ref, ct_ref, r_ref, rt_ref, wk_ref, wv_ref, q_own, q_oth, do_own, do_oth, *rest):
    (o_own, o_oth, dq_own, dq_oth, dkv_ref, dr_ref, dw_ref,
     w_s, k_s, kt_s, v_s, vt_s, qt_s, do_s, s_s, p_s, ds_s, o_s, dqt_s) = rest[n_alias:]
    d_n = v_s.shape[1]
    core = idx_ref[1]

    @pl.when(pl.program_id(0) == 0)
    def _():
        k_s[:, d_n:] = r_ref[...]
        kt_s[d_n:, :] = rt_ref[...]
        dr_ref[...] = rest[n_alias - 1][...] if n_alias else jnp.zeros(dr_ref.shape, F32)

    w_s[:, 0:d_n] = wk_ref[0]
    w_s[:, d_n:] = wv_ref[0]

    def at(i):
        return pl.ds(pl.multiple_of(i * PIECE, PIECE), PIECE)

    own_hi, own_lo, oth_hi, oth_lo = core, 3 - core, 1 - core, 2 + core
    lo, hi = pl.ds(0, PIECE), pl.ds(PIECE, PIECE)
    for pos, half, q_ref, do_ref in ((own_lo, lo, q_own, do_own), (own_hi, hi, q_own, do_own),
                                     (oth_lo, lo, q_oth, do_oth), (oth_hi, hi, q_oth, do_oth)):
        qt_s[:, at(pos)] = q_ref[0, :, half]
        do_s[at(pos), :] = do_ref[0, half, :]
    n_pieces = 4 * cp_half
    for chip in range(cp_half):
        dev_a, dev_b = 2 * chip, 2 * chip + 1
        lens = (n_pieces - dev_a, n_pieces - dev_b, dev_b + 1, dev_a + 1)
        pl.when(idx_ref[0] == chip)(functools.partial(
            head_body, lens, scale, c_ref, ct_ref, w_s, k_s, kt_s, v_s, vt_s, qt_s, do_s, s_s, p_s, ds_s,
            o_s, dqt_s, dw_ref, dkv_ref, dr_ref))
    for pos, half, o_ref, dq_ref in ((own_lo, lo, o_own, dq_own), (own_hi, hi, o_own, dq_own),
                                     (oth_lo, lo, o_oth, dq_oth), (oth_hi, hi, o_oth, dq_oth)):
        o_ref[0, half, :] = o_s[at(pos), :]
        dq_ref[0, :, half] = dqt_s[:, at(pos)]


sds = jax.ShapeDtypeStruct


def group_call(first, count, cp_half, scale, idx, c_all, ct_all, r_all, rt_all, w_k, w_v, q_all, q_oth, do_all, do_oth, carried):
    seq, rank = c_all.shape
    d_r = r_all.shape[1]
    half_heads, d_qk, tok = q_oth.shape
    d_v = do_oth.shape[2]
    kv = w_k.shape[2] + w_v.shape[2]
    whole = lambda *shape: pl.BlockSpec(shape, lambda h, idx: (0,) * len(shape), pipeline_mode=pl.Buffered(1))
    mine = lambda *shape: pl.BlockSpec((1,) + shape, lambda h, idx: (idx[1] * half_heads + first + h, 0, 0))
    part = lambda *shape: pl.BlockSpec((1,) + shape, lambda h, idx: (first + h, 0, 0))
    in_specs = [pl.BlockSpec(memory_space=pltpu.VMEM)] * 4 + [
                part(rank, w_k.shape[2]), part(rank, d_v), mine(d_qk, tok), part(d_qk, tok), part(tok, d_v), part(tok, d_v)]
    out_specs = [part(tok, d_v), part(tok, d_v), mine(d_qk, tok), part(d_qk, tok),
                 pl.BlockSpec((seq, kv), lambda h, idx: (0, first + h)),
                 pl.BlockSpec((seq, d_r), lambda h, idx: (0, 0)),
                 pl.BlockSpec((1, rank, kv), lambda h, idx: (h, 0, 0))]
    out_shape = [sds((half_heads, tok, d_v), BF16), sds((half_heads, tok, d_v), BF16),
                 sds((2 * half_heads, d_qk, tok), F32), sds((half_heads, d_qk, tok), F32),
                 sds((seq, half_heads * kv), BF16), sds((seq, d_r), F32), sds((count, rank, kv), F32)]
    args = [idx, c_all, ct_all, r_all, rt_all, w_k, w_v, q_all, q_oth, do_all, do_oth]
    aliases = {}
    for i, arr in enumerate(carried):
        aliases[len(args)] = i
        args.append(arr)
        in_specs.append(pl.BlockSpec(memory_space=pl.ANY))
    if carried:
        in_specs[-1] = whole(seq, d_r)
    pairs = 2 * tok * (seq // 2 + PIECE // 2)
    flops = count * (2 * pairs * (3 * d_qk + 3 * d_v) + 6 * seq * rank * kv)
    return pl.pallas_call(
        functools.partial(group_kernel, cp_half, scale, len(carried)),
        grid_spec=pltpu.PrefetchScalarGridSpec(
            num_scalar_prefetch=1, grid=(count,), in_specs=in_specs, out_specs=out_specs,
            scratch_shapes=[
                pltpu.VMEM((rank, kv), BF16),
                pltpu.VMEM((seq, d_qk), BF16), pltpu.VMEM((d_qk, seq), BF16),
                pltpu.VMEM((seq, d_v), BF16), pltpu.VMEM((d_v, seq), BF16),
                pltpu.VMEM((d_qk, 2 * tok), BF16), pltpu.VMEM((2 * tok, d_v), BF16),
                pltpu.VMEM((seq * 2 + 2 * PIECE, PIECE), F32),
                pltpu.VMEM((seq, 2 * tok), BF16), pltpu.VMEM((seq, 2 * tok), BF16),
                pltpu.VMEM((2 * tok, d_v), BF16), pltpu.VMEM((d_qk, 2 * tok), F32)]),
        out_shape=out_shape,
        input_output_aliases=aliases,
        compiler_params=params(57),
        cost_estimate=pl.CostEstimate(flops=int(flops), bytes_accessed=count * 4 * 2 ** 20, transcendentals=count * pairs),
        name="heads",
    )(*args)


def dc_kernel(idx_ref, lo_ref, hi_ref, wk_ref, wv_ref, dr_lo, dr_hi, *refs):
    sends, keeps, w_s = refs[0:2], refs[2:4], refs[4]
    heads, rank, d_n = wk_ref.shape
    i = pl.program_id(0)

    @pl.when(i == 0)
    def _():
        for g in range(heads):
            w_s[:, 2 * g * d_n:(2 * g + 1) * d_n] = wk_ref[g]
            w_s[:, (2 * g + 1) * d_n:(2 * g + 2) * d_n] = wv_ref[g]

    def fill(outs):
        wide, slim = outs
        split = wide.shape[3]
        for k, (dkv_ref, dr_ref) in enumerate(((lo_ref, dr_lo), (hi_ref, dr_hi))):
            for j in range(0, rank, PIECE):
                dc = dot_t(dkv_ref[...], w_s[j:j + PIECE, :])
                n_wide = min(split - j, PIECE)
                wide[0, k, :, j:j + n_wide] = dc[:, :n_wide]
                if n_wide < PIECE:
                    slim[0, k, :, 0:rank - split] = dc[:, n_wide:]
            dr = dr_ref[...]
            slim[0, k, :, rank - split:] = jnp.concatenate([dr, jnp.zeros_like(dr)], axis=1)

    pl.when(i < 2)(functools.partial(fill, sends))
    pl.when(i >= 2)(functools.partial(fill, keeps))


def dc_call(split, idx, dkv, w_k, w_v, dr):
    seq, d_r = dr.shape
    half_heads, rank, d_n = w_k.shape
    kv = d_n + w_v.shape[2]
    n = seq // (2 * PIECE)
    dev = lambda i, idx: 2 * (i % 2) + jnp.where(i < 2, 1 - idx[1], idx[1])
    lo = lambda w: pl.BlockSpec((PIECE, w), lambda i, idx: (dev(i, idx), 0))
    hi = lambda w: pl.BlockSpec((PIECE, w), lambda i, idx: (2 * n - 1 - dev(i, idx), 0))
    w_spec = pl.BlockSpec((half_heads, rank, d_n), lambda i, idx: (0, 0, 0), pipeline_mode=pl.Buffered(1))
    shapes = [(n // 2, 2, PIECE, split), (n // 2, 2, PIECE, rank - split + 2 * d_r)] * 2
    maps = [lambda i, idx: (jnp.minimum(i, 1), 0, 0, 0)] * 2 + [lambda i, idx: (jnp.maximum(i - 2, 0), 0, 0, 0)] * 2
    return pl.pallas_call(
        dc_kernel,
        grid_spec=pltpu.PrefetchScalarGridSpec(
            num_scalar_prefetch=1, grid=(n,),
            in_specs=[lo(half_heads * kv), hi(half_heads * kv), w_spec, w_spec, lo(d_r), hi(d_r)],
            out_specs=[pl.BlockSpec((1,) + s[1:], m) for s, m in zip(shapes, maps)],
            scratch_shapes=[pltpu.VMEM((rank, half_heads * kv), BF16)]),
        out_shape=[sds(s, F32) for s in shapes],
        compiler_params=params(60),
        cost_estimate=pl.CostEstimate(flops=2 * seq * rank * kv * half_heads, bytes_accessed=30 * 2 ** 20, transcendentals=0),
        name="dc",
    )(idx, dkv, dkv, w_k, w_v, dr, dr)


def gather_kernel(n_dev, idx_ref, *refs):
    c_refs, r_refs = refs[0:4], refs[4:8]
    c_all, ct_all, r_all, rt_all = refs[8:]
    chip, core = idx_ref[0], idx_ref[1]
    devs = (2 * chip + core, 2 * chip + 1 - core, 2 - 2 * chip + core, 3 - 2 * chip - core)
    for dev, c_ref, r_ref in zip(devs, c_refs, r_refs):
        for piece, half in ((dev, rows(0)), (2 * n_dev - 1 - dev, rows(1))):
            at = pl.ds(pl.multiple_of(piece * PIECE, PIECE), PIECE)
            c = c_ref[half, :]
            c_all[at, :] = c
            ct_all[:, at] = c.T
            r = r_ref[:, half]
            rt_all[:, at] = r
            r_all[at, :] = r.T


def gather_call(idx, n_dev, c_parts, r_parts):
    tok, rank = c_parts[0].shape
    d_r = r_parts[0].shape[0]
    seq = n_dev * tok
    whole = lambda shape: pl.BlockSpec(shape, lambda i, idx: (0, 0))
    shapes = [(seq, rank), (rank, seq), (seq, d_r), (d_r, seq)]
    return pl.pallas_call(
        functools.partial(gather_kernel, n_dev),
        grid_spec=pltpu.PrefetchScalarGridSpec(
            num_scalar_prefetch=1, grid=(1,),
            in_specs=[whole((tok, rank))] * 4 + [whole((d_r, tok))] * 4,
            out_specs=[pl.BlockSpec(memory_space=pltpu.VMEM)] * 4),
        out_shape=[pltpu.VMEM(s, BF16) for s in shapes],
        compiler_params=params(40),
        cost_estimate=pl.CostEstimate(flops=10 ** 9, bytes_accessed=8 * 2 ** 20, transcendentals=0),
        name="gather",
    )(idx, *c_parts, *r_parts)


def relay_kernel(idx_ref, *refs):
    n = len(refs) // 2
    for in_ref, out_ref in zip(refs[:n], refs[n:]):
        out_ref[...] = jnp.swapaxes(in_ref[...], 0, 1)


def relay_call(idx, w_uk, w_uv, d_out):
    tok, n_heads, d = d_out.shape
    heads = n_heads // 2
    n = 256
    near = pl.BlockSpec((n, heads, d), lambda i, idx: (i, idx[1], 0))
    away = pl.BlockSpec((n, heads, d), lambda i, idx: (i, 1 - idx[1], 0))
    return pl.pallas_call(
        relay_kernel,
        grid_spec=pltpu.PrefetchScalarGridSpec(
            num_scalar_prefetch=1, grid=(tok // n,), in_specs=[away, near, near, near],
            out_specs=[pl.BlockSpec((heads, n, d), lambda i, idx: (0, i, 0))] * 4),
        out_shape=[sds((heads, tok, d), BF16)] * 4,
        compiler_params=params(60),
        cost_estimate=pl.CostEstimate(flops=10 ** 9, bytes_accessed=16 * d_out.size, transcendentals=0),
        name="relay",
    )(idx, d_out, d_out, w_uk, w_uv)


def out_kernel(idx_ref, own_ref, oth_ref, out_ref):
    core = idx_ref[1]
    heads = own_ref.shape[0]
    for side, ref in ((core, own_ref), (1 - core, oth_ref)):
        out_ref[:, pl.ds(pl.multiple_of(side * heads, heads), heads), :] = jnp.swapaxes(ref[...], 0, 1)


def out_call(idx, own, oth):
    heads, tok, d = own.shape
    n = 256
    part = pl.BlockSpec((heads, n, d), lambda i, idx: (0, i, 0))
    return pl.pallas_call(
        out_kernel,
        grid_spec=pltpu.PrefetchScalarGridSpec(
            num_scalar_prefetch=1, grid=(tok // n,), in_specs=[part, part],
            out_specs=pl.BlockSpec((n, 2 * heads, d), lambda i, idx: (i, 0, 0))),
        out_shape=sds((tok, 2 * heads, d), BF16),
        compiler_params=params(60),
        cost_estimate=pl.CostEstimate(flops=10 ** 9, bytes_accessed=4 * own.size * 2, transcendentals=0),
        name="out",
    )(idx, own, oth)


def place_kernel(idx_ref, part_ref, full_ref, out_ref):
    out_ref[...] = part_ref[...]


def place_call(idx, part, full, step):
    n, a, b = part.shape
    return pl.pallas_call(
        place_kernel,
        grid_spec=pltpu.PrefetchScalarGridSpec(
            num_scalar_prefetch=1, grid=(n // step,),
            in_specs=[pl.BlockSpec((step, a, b), lambda h, idx: (h, 0, 0)), pl.BlockSpec(memory_space=pl.ANY)],
            out_specs=pl.BlockSpec((step, a, b), lambda h, idx: ((1 - idx[1]) * (n // step) + h, 0, 0))),
        out_shape=sds(full.shape, full.dtype),
        input_output_aliases={2: 0},
        compiler_params=params(60),
        cost_estimate=pl.CostEstimate(flops=10 ** 9, bytes_accessed=2 * part.size * part.dtype.itemsize, transcendentals=0),
        name="place",
    )(idx, part, full)


def join_kernel(n_parts, idx_ref, *refs):
    a_refs, b_refs = refs[:n_parts], refs[n_parts:2 * n_parts]
    k_ref, v_ref = refs[-2:]
    n_rows, heads, d_n = k_ref.shape
    h = 0
    for a_ref, b_ref in zip(a_refs, b_refs):
        for g in range(a_ref.shape[0]):
            s = a_ref[g] + b_ref[g]
            at = pl.ds(h, n_rows, stride=heads)
            k_ref.reshape(n_rows * heads, d_n)[at, :] = s[:, :d_n]
            v_ref.reshape(n_rows * heads, d_n)[at, :] = s[:, d_n:]
            h += 1


def join_call(idx, block, parts_a, parts_b, carried, n_heads):
    rank, kv = parts_a[0].shape[1:]
    n_parts = len(parts_a)
    heads = sum(p.shape[0] for p in parts_a)
    r_blk = 256
    parts = [pl.BlockSpec((p.shape[0], r_blk, kv), lambda i, idx: (0, i, 0)) for p in parts_a]
    out = pl.BlockSpec((r_blk, heads, kv // 2), lambda i, idx: (i, block(idx[1]), 0))
    args = [idx, *parts_a, *parts_b, *carried]
    return pl.pallas_call(
        functools.partial(join_kernel, n_parts),
        grid_spec=pltpu.PrefetchScalarGridSpec(
            num_scalar_prefetch=1, grid=(rank // r_blk,),
            in_specs=parts + parts + [pl.BlockSpec(memory_space=pl.ANY)] * len(carried),
            out_specs=[out, out]),
        out_shape=[sds((rank, n_heads, kv // 2), F32)] * 2,
        input_output_aliases={1 + 2 * n_parts + i: i for i in range(len(carried))},
        compiler_params=params(60),
        cost_estimate=pl.CostEstimate(flops=10 ** 9, bytes_accessed=3 * heads * rank * kv * 4, transcendentals=0),
        name="join",
    )(*args)


def solution(mesh):
    n_cp = mesh.shape['cp']
    n_tp = mesh.shape['tp']
    cp_half = n_cp // 2
    x_perm = [(d, (d + 2) % n_cp) for d in range(n_cp)]
    core_perm = [(d, d ^ 1) for d in range(n_cp)]
    tp_perm = [(d, (d + 1) % n_tp) for d in range(n_tp)]
    seq_spec = P(('dp', 'cp'), None)
    head_spec = P(('dp', 'cp'), 'tp', None)
    weight_spec = P(None, 'tp', None)
    grad_spec = P('dp', 'tp', None)

    def device_fn(c_latent, k_rope, q_heads, d_out, w_uk, w_uv):
        _, rank = c_latent.shape
        n_heads = q_heads.shape[1]
        half_heads = n_heads // 2
        d_r = k_rope.shape[1]
        d_n = w_uk.shape[2]
        scale = q_heads.shape[2] ** -0.5
        me = lax.axis_index('cp')
        chip, core = me // 2, me % 2
        my_tp = lax.axis_index('tp')
        swap_x = lambda a: lax.ppermute(a, 'cp', x_perm)
        swap_core = lambda a: lax.ppermute(a, 'cp', core_perm)
        swap_tp = lambda a: lax.ppermute(a, 'tp', tp_perm)

        def parts(own):
            far = swap_x(own)
            return own, swap_core(own), far, swap_core(far)

        idx = jnp.stack([chip, core]).astype(jnp.int32)
        c_all, ct_all, r_all, rt_all = gather_call(idx, n_cp, parts(c_latent), parts(k_rope.T))
        c_all, ct_all, r_all, rt_all = (pltpu.with_memory_space_constraint(a, pltpu.VMEM) for a in (c_all, ct_all, r_all, rt_all))
        do_send, do_all, w_k, w_v = relay_call(idx, w_uk, w_uv, d_out)
        q_all = q_heads.transpose(1, 2, 0)
        away = (1 - core) * half_heads
        q_oth = swap_core(lax.dynamic_slice_in_dim(q_all, away, half_heads, 0))
        do_oth = swap_core(do_send)

        carried, own, far, near, far_near = (), [], [], [], []
        first = 0
        for count in sum(GROUPS, ()):
            outs = group_call(first, count, cp_half, scale, idx, c_all, ct_all, r_all, rt_all, w_k, w_v,
                      q_all, q_oth, do_all, do_oth, carried)
            carried = outs[:6]
            own.append(outs[6])
            far.append(swap_x(outs[6]))
            near.append(swap_core(outs[6]))
            far_near.append(swap_core(far[-1]))
            first += count
        o_own, o_oth, dq_full, dq_oth, dkv, dr = carried

        def fold(arrs, axis, pos, swap):
            cut = lambda p: [lax.dynamic_index_in_dim(a, p, axis, keepdims=False) for a in arrs]
            return cut(pos) + [swap(functools.reduce(jnp.add, cut(1 - pos)))]

        full = []
        split = rank - d_n
        dc_out = dc_call(split, idx, dkv, w_k, w_v, dr)
        for half in range(2):
            arrs = [dc_out[2 + half], swap_core(dc_out[half])]
            arrs = fold(arrs, 1, my_tp, swap_tp)
            part = functools.reduce(jnp.add, fold(arrs, 0, chip, swap_x))
            mate = swap_tp(part)
            full.append(jnp.where(my_tp == 0, jnp.concatenate([part, mate], axis=0), jnp.concatenate([mate, part], axis=0)))
        dc = jnp.concatenate([full[0], full[1][:, :rank - split]], axis=1)
        dr_out = full[1][:, rank - split:rank - split + d_r]

        dws, g0 = (), 0
        for i, groups in enumerate(GROUPS):
            sel = slice(g0, g0 + len(groups))
            g0 += len(groups)
            for s, (a, b) in enumerate(((own, far), (near, far_near))):
                block = lambda c, i=i, s=s: (1 - c if s else c) * len(GROUPS) + i
                dws = join_call(idx, block, a[sel], b[sel], dws, n_heads)
        dq = place_call(idx, swap_core(dq_oth), dq_full, 8).transpose(2, 0, 1)
        out = out_call(idx, o_own, swap_core(o_oth))
        return (out, dq, dc, dr_out, *dws)

    return jax.shard_map(device_fn, mesh=mesh,
                         in_specs=(seq_spec, seq_spec, head_spec, head_spec, weight_spec, weight_spec),
                         out_specs=(head_spec, head_spec, seq_spec, seq_spec, grad_spec, grad_spec),
                         check_vma=False)
```
